512 devices in a mesh: leaf: 512 (over x, y, z, core).
Axes of the slice: x: 4, y: 8, z: 8, core: 2. Of those that a mesh axis runs over, the one named last changes fastest.
Arguments:
- vectors: float32 [16, 2097152], P(None, 'leaf'), may hold values from -6 to 6
- morton_order: int32 [512, 4096], P('leaf'), may hold values from 0 to 4095, each once within a row
- leaf_sizes: int32 [512, 32], P('leaf'), may hold values from 1 to 256, 4096 in all within a row
- leaf_basis: bfloat16 [32, 2097152], P(None, 'leaf'), may hold values from -0.5 to 0.5
- leaf_transfer: bfloat16 [16384, 1024], P('leaf'), may hold values from -0.75 to 0.75
- mid_transfer: bfloat16 [2048, 1024], P('leaf'), may hold values from -1 to 1
- root_transfer: bfloat16 [512, 1024], P('leaf'), may hold values from -0.75 to 0.75
- leaf_pairs: int32 [2, 32768], P(None, 'leaf'), may hold values from 0 to 31, as said below
- leaf_coupling: bfloat16 [32768, 1024], P('leaf'), may hold values from -0.5 to 0.5
- dev_partner: int32 [512, 128], P('leaf'), may hold values from -1 to 511, as said below
- dev_coupling: bfloat16 [65536, 1024], P('leaf'), may hold values from -0.25 to 0.25
- grp_partner: int32 [512, 4], P('leaf'), may hold values from 0 to 63, as said below
- grp_coupling: bfloat16 [2048, 1024], P('leaf'), may hold values from -0.5 to 0.5
Outputs:
- far_field: float32 [16, 2097152], P(None, 'leaf')
The draws below stay inside these ranges and needn't reach their ends.
Inputs may be any that keep to these rules, and one draw needn't show every extreme that they name: `morton_order`: each row is a permutation of 0 to 4095. `leaf_pairs`: the two leaves of a pair differ. `dev_partner`: live entries of a row come first, are distinct and never the row's own subtree; an unordered pair of subtrees appears in at most one slot of all rows; some row has all 128 slots live. `grp_partner`: never the device's own group.
All inputs are finite; a program needn't handle non-finite values.
Results may differ from the reference program's by a relative error of at most 0.014.
Values may be sent and summed in bfloat16 or wider, within the bound.
A program may use at most 64 MiB of HBM per device.

```python
import math
import jax
import jax.numpy as jnp
import numpy as np
from jax import lax

RANK = 32
LEAF = 256
VECS = 16
LEAVES_DEV = 32
LPAIRS = 64
GCAP = 4
PTS_DEV = 4096
MIDS_DEV = 4
SUBTREES = 512
GROUPS = 64
PCAP = 128
POINTS = 2097152
LEAVES = 16384
MIDS = 2048


def draw_leaf_pairs(key, part):
    base_key = jax.random.fold_in(key, 31)
    first_key, step_key = jax.random.split(base_key)
    first_leaf = jax.random.randint(first_key, (SUBTREES * LPAIRS,), 0, LEAVES_DEV)
    offset = jax.random.randint(step_key, (SUBTREES * LPAIRS,), 1, LEAVES_DEV)
    second = (first_leaf + offset) % LEAVES_DEV
    return jnp.stack([first_leaf, second]).astype(jnp.int32)


def draw_grp_partner(key, part):
    base_key = jax.random.fold_in(key, 47)
    offset = jax.random.randint(base_key, (SUBTREES, GCAP), 1, GROUPS)
    own_group = (jnp.arange(SUBTREES, dtype=jnp.int32) // 8)[:, None]
    return ((own_group + offset) % GROUPS).astype(jnp.int32)


def draw_dev_partner(key, part):
    base_key = jax.random.fold_in(key, 59)
    perm_key, score_key, count_key = jax.random.split(base_key, 3)
    ranking = jax.random.permutation(perm_key, SUBTREES).astype(jnp.int32)
    scores = jax.random.randint(score_key, (SUBTREES, SUBTREES), 0, 1 << 20) * SUBTREES + jnp.arange(SUBTREES, dtype=jnp.int32)[None, :]
    allowed = ranking[None, :] > ranking[:, None]
    scores = jnp.where(allowed, scores, -1)
    top_score, top_index = lax.top_k(scores, PCAP)
    counts = jax.random.randint(count_key, (SUBTREES,), 1, PCAP + 1)
    counts = jnp.where(ranking == 0, PCAP, counts)
    slots = jnp.arange(PCAP, dtype=jnp.int32)[None, :]
    is_live = (top_score >= 0) & (slots < counts[:, None])
    return jnp.where(is_live, top_index, -1).astype(jnp.int32)


def level_of(stream_key, shape, cuts, low, top_value):
    factor_of, own = 1.0, jax.random.fold_in(stream_key, 6)
    for position, blocks in cuts:
        heights = jnp.exp(jax.random.uniform(jax.random.fold_in(own, position), (blocks,), jnp.float32, low / len(cuts), top_value / len(cuts)))
        factor_of = factor_of * jnp.repeat(heights, shape[position] // blocks).reshape([-1 if axis == position else 1 for axis in range(len(shape))])
    return factor_of


def length_profile(amount, total, reach, slope):
    weights = [(1 << 20) // math.isqrt(rank ** slope) + 1 for rank in range(2, amount + 1)]
    spare, given = total - reach - (amount - 1), [1] * (amount - 1)
    while spare > 0:
        candidates = [i for i in range(amount - 1) if given[i] < reach]
        mass, budget = sum([weights[i] for i in candidates]), spare
        for i in candidates:
            more = min(reach - given[i], max(1, budget * weights[i] // mass), spare)
            given[i] = given[i] + more
            spare = spare - more
    return np.array([reach] + given)


def uneven_parts(stream_key, amount, total, limit, skew):
    if amount == 2:
        one = jax.random.randint(stream_key, (), max(1, total - limit), min(limit, total - 1) + 1)
        return jnp.stack([one, total - one])
    lengths = jnp.asarray(length_profile(amount, total, limit, skew), jnp.int32)
    twos = (amount - 1) // 2
    donor, taker = lengths[1:1 + 2 * twos:2], lengths[2:2 + 2 * twos:2]
    room = jnp.minimum(donor - 1, limit - taker)
    shifted = jax.random.randint(jax.random.fold_in(stream_key, 1), (twos,), 0, 1 << 20) % (room + 1)
    lengths = lengths.at[1:1 + 2 * twos:2].set(donor - shifted).at[2:2 + 2 * twos:2].set(taker + shifted)
    return lengths[jax.random.permutation(jax.random.fold_in(stream_key, 2), amount)]


def scatter_about(rng, dims, deviation, bound, pieces=(), kind=jnp.bfloat16):
    values = deviation * jax.random.normal(rng, dims, jnp.float32)
    if pieces:
        values = values * level_of(rng, dims, pieces, -0.22, 0.18)
    return jnp.clip(values, -bound, bound).astype(kind)


def setup_inputs(seed: int = 0) -> dict:
    seeds = jax.random.split(jax.random.key(seed), 14)
    vectors = scatter_about(seeds[0], (VECS, POINTS), 1.0, 6.0, ((1, 512),), jnp.float32)
    morton_order = jax.vmap(lambda own: jax.random.permutation(own, PTS_DEV))(jax.random.split(seeds[1], SUBTREES)).reshape((SUBTREES, PTS_DEV)).astype(jnp.int32)
    leaf_sizes = jax.vmap(lambda own: uneven_parts(own, LEAVES_DEV, PTS_DEV, LEAF, 1))(jax.random.split(seeds[2], SUBTREES)).reshape((SUBTREES, LEAVES_DEV)).astype(jnp.int32)
    leaf_basis = scatter_about(seeds[3], (RANK, POINTS), (LEAF // 2) ** -0.5, 0.5, ((1, 512),))
    leaf_transfer = scatter_about(seeds[4], (LEAVES, RANK * RANK), (2 * RANK) ** -0.5, 0.75, ((0, 512),))
    mid_transfer = scatter_about(seeds[5], (MIDS, RANK * RANK), (RANK * MIDS_DEV // 4) ** -0.5, 1.0, ((0, 512),))
    root_transfer = scatter_about(seeds[6], (SUBTREES, RANK * RANK), (2 * RANK) ** -0.5, 0.75, ((0, 512),))
    leaf_pairs = draw_leaf_pairs(jax.random.fold_in(seeds[13], 71), 0)
    leaf_coupling = scatter_about(seeds[8], (SUBTREES * LPAIRS, RANK * RANK), (4 * RANK) ** -0.5, 0.5, ((0, 512),))
    dev_partner = draw_dev_partner(jax.random.fold_in(seeds[13], 71), 0)
    dev_coupling = scatter_about(seeds[10], (SUBTREES * PCAP, RANK * RANK), (16 * RANK) ** -0.5, 0.25, ((0, 512),))
    grp_partner = draw_grp_partner(jax.random.fold_in(seeds[13], 71), 0)
    grp_coupling = scatter_about(seeds[12], (SUBTREES * GCAP, RANK * RANK), (4 * RANK) ** -0.5, 0.5, ((0, 512),))
    return {"vectors": vectors, "morton_order": morton_order, "leaf_sizes": leaf_sizes, "leaf_basis": leaf_basis, "leaf_transfer": leaf_transfer, "mid_transfer": mid_transfer, "root_transfer": root_transfer, "leaf_pairs": leaf_pairs, "leaf_coupling": leaf_coupling, "dev_partner": dev_partner, "dev_coupling": dev_coupling, "grp_partner": grp_partner, "grp_coupling": grp_coupling}


def rounded(value):
    return lax.optimization_barrier(value.astype(jnp.bfloat16)).astype(jnp.float32)


def windows(sizes, total):
    starts = jnp.cumsum(sizes) - sizes
    offset = jnp.arange(LEAF, dtype=jnp.int32)
    places = starts[:, None] + offset[None, :]
    inside = offset[None, :] < sizes[:, None]
    return jnp.minimum(places, total - 1).astype(jnp.int32), inside


def reference(vectors, morton_order, leaf_sizes, leaf_basis, leaf_transfer, mid_transfer, root_transfer, leaf_pairs, leaf_coupling, dev_partner, dev_coupling, grp_partner, grp_coupling):
    subtrees = morton_order.shape[0]
    points = morton_order.shape[1]
    count_vec = vectors.shape[0]
    basis_rank = leaf_basis.shape[0]
    leaves = leaf_sizes.shape[1]
    middle = leaves // 8
    groups = subtrees // 8
    vec_dev = vectors.reshape(count_vec, subtrees, points).transpose(1, 0, 2)
    basis_dev = leaf_basis.reshape(basis_rank, subtrees, points).transpose(1, 0, 2)
    leaf_maps = leaf_transfer.reshape(subtrees, leaves, basis_rank, basis_rank)
    mid_maps = mid_transfer.reshape(subtrees, middle, basis_rank, basis_rank)
    root_maps = root_transfer.reshape(subtrees, basis_rank, basis_rank).astype(jnp.float32)
    pairs_dev = leaf_pairs.reshape(2, subtrees, -1).transpose(1, 0, 2)
    leaf_blocks = leaf_coupling.reshape(subtrees, -1, basis_rank, basis_rank)

    def upward(device_item):
        vec, morton, sizes, basis, lmap, mmap, rmap, pairs, blocks = device_item
        places, inside = windows(sizes, points)
        sorted_vec = vec[:, morton].astype(jnp.bfloat16).astype(jnp.float32)
        basis_win = basis[:, places].astype(jnp.float32)
        vec_win = jnp.where(inside[None], sorted_vec[:, places], 0.0)
        leaf_coeff = rounded(jnp.einsum("rls,vls->lrv", basis_win, vec_win))
        child = jnp.einsum("lij,liv->ljv", lmap.astype(jnp.float32), leaf_coeff)
        mid_coeff = rounded(child.reshape(middle, 8, basis_rank, count_vec).sum(1))
        root_coeff = rounded(jnp.einsum("mij,miv->jv", mmap.astype(jnp.float32), mid_coeff))
        group_term = rounded(jnp.einsum("ij,iv->jv", rmap, root_coeff))
        blockf = blocks.astype(jnp.float32)
        forward = jnp.einsum("pij,pjv->piv", blockf, leaf_coeff[pairs[1]])
        backward = jnp.einsum("pij,piv->pjv", blockf, leaf_coeff[pairs[0]])
        leaf_far = jnp.zeros((leaves, basis_rank, count_vec), jnp.float32)
        leaf_far = leaf_far.at[pairs[0]].add(forward).at[pairs[1]].add(backward)
        return root_coeff, group_term, leaf_far

    root_coeff, group_term, leaf_far = lax.map(upward, (vec_dev, morton_order, leaf_sizes, basis_dev, leaf_maps, mid_maps, root_maps, pairs_dev, leaf_blocks))
    group_coeff = rounded(group_term.reshape(groups, 8, basis_rank, count_vec).sum(1))
    is_live = dev_partner >= 0
    safe_id = jnp.where(is_live, dev_partner, 0).astype(jnp.int32)
    dev_blocks = dev_coupling.reshape(subtrees, -1, basis_rank, basis_rank).astype(jnp.float32)
    chosen = root_coeff[safe_id] * is_live[..., None, None].astype(jnp.float32)
    root_far = jnp.einsum("acij,acjv->aiv", dev_blocks, chosen)
    back = jnp.einsum("acij,aiv->acjv", dev_blocks, root_coeff) * is_live[..., None, None].astype(jnp.float32)
    root_far = root_far.at[safe_id.reshape(-1)].add(back.reshape(-1, basis_rank, count_vec))
    own_group = (jnp.arange(subtrees, dtype=jnp.int32) // 8).astype(jnp.int32)
    grp_blocks = grp_coupling.reshape(subtrees, -1, basis_rank, basis_rank).astype(jnp.float32)
    to_own = jnp.einsum("acij,acjv->aiv", grp_blocks, group_coeff[grp_partner])
    to_far = jnp.einsum("acij,aiv->acjv", grp_blocks, group_coeff[own_group])
    group_far = jnp.zeros((groups, basis_rank, count_vec), jnp.float32)
    group_far = rounded(group_far.at[own_group].add(to_own).at[grp_partner.reshape(-1)].add(to_far.reshape(-1, basis_rank, count_vec)))
    root_total = rounded(root_far + jnp.einsum("aij,ajv->aiv", root_maps, group_far[own_group]))

    def downward(device_item):
        morton, sizes, basis, lmap, mmap, top, near = device_item
        places, inside = windows(sizes, points)
        mid_total = rounded(jnp.einsum("mij,jv->miv", mmap.astype(jnp.float32), top))
        parent = jnp.repeat(mid_total, 8, axis=0)
        leaf_total = rounded(near + jnp.einsum("lij,ljv->liv", lmap.astype(jnp.float32), parent))
        basis_win = basis[:, places].astype(jnp.float32)
        out_win = jnp.where(inside[None], jnp.einsum("rls,lrv->vls", basis_win, leaf_total), 0.0)
        sorted_out = jnp.zeros((count_vec, points), jnp.float32).at[:, places].add(out_win)
        return jnp.zeros((count_vec, points), jnp.float32).at[:, morton].set(sorted_out)

    result = lax.map(downward, (morton_order, leaf_sizes, basis_dev, leaf_maps, mid_maps, root_total, leaf_far))
    return result.transpose(1, 0, 2).reshape(count_vec, subtrees * points)
```

```python
import jax
import jax.numpy as jnp
from jax import lax
from jax.experimental import pallas as pl
from jax.experimental.pallas import tpu as pltpu
from jax.sharding import Mesh
from jax.sharding import PartitionSpec as P

LEAF = 256
LEAF_AXES = ("leaf_0", "leaf_1", "leaf_2", "leaf_3")


F32, BF16, I32 = jnp.float32, jnp.bfloat16, jnp.int32
NT = (((1,), (1,)), ((), ()))
TN = (((0,), (0,)), ((), ()))


def iota(shape, dim):
    return lax.broadcasted_iota(I32, shape, dim)


def dot(a, b, dims=(((1,), (0,)), ((), ()))):
    return lax.dot_general(a, b, dims, preferred_element_type=F32)


def hot(mask):
    return jnp.where(mask, 1.0, 0.0).astype(BF16)


def spread_row():
    return hot(iota((32, 1024), 1) // 32 == iota((32, 1024), 0))


def spread_col():
    return hot(iota((32, 1024), 1) % 32 == iota((32, 1024), 0))


def fold_first(x):
    w = x[:, 0:128]
    for q in range(1, 8):
        w = w + x[:, q * 128 : (q + 1) * 128]
    return (w[:, 0:32] + w[:, 32:64]) + (w[:, 64:96] + w[:, 96:128])


def leaf_of(siz_ref, start, width):
    sizes = siz_ref[...].astype(F32)
    lower = iota((32, 32), 1) <= iota((32, 32), 0)
    ends = jnp.sum(jnp.where(lower, jnp.broadcast_to(sizes, (32, 32)), 0.0), axis=1, keepdims=True)
    pos = (iota((32, width), 1) + start).astype(F32)
    return jnp.sum(jnp.where(pos >= ends, 1.0, 0.0), axis=0, keepdims=True)


CH = 256


def up_kernel(vec, mor, siz, bas, lt, mt, rt, lc_out, root_out, term_out, masked, lt32):
    lt32[...] = lt[...].astype(F32)
    vx = jnp.concatenate([vec[:, h * 256 : (h + 1) * 256] for h in range(16)], axis=0).astype(BF16)

    def chunk(c, carry):
        at = pl.multiple_of(c * CH, CH)
        m = mor[:, pl.ds(at, CH)]
        lo, hi = m & 255, m >> 8
        pick = hot(iota((256, CH), 0) == lo)
        wide = dot(vx, pick)
        hib = jnp.broadcast_to(hi, (16, CH))
        sv = wide[0:16]
        for h in range(1, 16):
            sv = jnp.where(hib == h, wide[h * 16 : (h + 1) * 16], sv)
        leaf = jnp.broadcast_to(leaf_of(siz, at, CH), (16, CH)).astype(BF16)
        svb = sv.astype(BF16)
        for l in range(32):
            masked[l * 16 : (l + 1) * 16, pl.ds(at, CH)] = jnp.where(leaf == l, svb, jnp.zeros((), BF16))
        return carry

    lax.fori_loop(0, 4096 // CH, chunk, 0)
    lc = dot(masked[...], bas[...], NT).astype(BF16)
    lc_out[...] = lc
    erow = spread_row()
    root = jnp.zeros((16, 1024), F32)
    for m in range(4):
        acc = jnp.zeros((16, 1024), F32)
        x = dot(lc[m * 128 : (m + 1) * 128], erow)
        for l in range(8):
            acc = acc + x[l * 16 : (l + 1) * 16] * lt32[m * 8 + l : m * 8 + l + 1, :]
        mid = fold_first(acc).astype(BF16)
        root = root + dot(mid, erow) * mt[m : m + 1, :].astype(F32)
    root = fold_first(root).astype(BF16)
    root_out[...] = root
    term_out[...] = fold_first(dot(root, erow) * rt[...].astype(F32)).astype(BF16)


def pair_kernel(idx, lc, pairs, coup, far_out, s32, got, fwd, bwd):
    s32[...] = coup[...].astype(F32)
    erow, ecol = spread_row(), spread_col()
    back = hot(iota((1024, 32), 0) // 32 == iota((1024, 32), 1))

    def group(g, carry):
        for which, e in ((1, ecol), (0, erow)):
            for k in range(8):
                b = idx[which, g * 8 + k]
                got[k * 16 : (k + 1) * 16, :] = lc[pl.ds(pl.multiple_of(b * 16, 16), 16), :]
            x = dot(got[...], e)
            parts = [x[k * 16 : (k + 1) * 16] * s32[pl.ds(g * 8 + k, 1), :] for k in range(8)]
            if which == 1:
                y = dot(jnp.concatenate(parts, axis=0).astype(BF16), back)
                fwd[pl.ds(pl.multiple_of(g * 128, 128), 128), :] = y.astype(BF16)
            else:
                y = jnp.concatenate([fold_first(t) for t in parts], axis=0)
                bwd[pl.ds(pl.multiple_of(g * 128, 128), 128), :] = y.astype(BF16)
        return carry

    lax.fori_loop(0, 8, group, 0)
    wide = hot(iota((64, 1024), 1) // 16 == iota((64, 1024), 0))
    ids = dot(pairs[...].astype(F32).astype(BF16), wide)
    same = iota((512, 1024), 0) % 16 == iota((512, 1024), 1) % 16
    leaf = (iota((512, 1024), 0) // 16).astype(F32)
    far_out[...] = dot(hot(same & (leaf == ids[0:1])), fwd[...]) + dot(hot(same & (leaf == ids[1:2])), bwd[...])


def down_kernel(top, far, mor, siz, bas, lt, mt, out, scat):
    erow, ecol = spread_row(), spread_col()
    back = hot(iota((1024, 32), 0) // 32 == iota((1024, 32), 1))
    xt = dot(top[...], ecol)
    p = jnp.concatenate([xt * mt[m : m + 1, :].astype(F32) for m in range(4)], axis=0)
    ph = p.astype(BF16)
    pl_ = (p - ph.astype(F32)).astype(BF16)
    mid = (dot(ph, back) + dot(pl_, back)).astype(BF16)
    tots = []
    for m in range(4):
        x = dot(mid[m * 16 : (m + 1) * 16], ecol)
        q = jnp.concatenate(
            [x * lt[m * 8 + l : m * 8 + l + 1, :].astype(F32) for l in range(8)], axis=0
        ).astype(BF16)
        tots.append((dot(q, back) + far[m * 128 : (m + 1) * 128, :]).astype(BF16))
    tot = jnp.concatenate(tots, axis=0)

    def chunk(c, acc):
        at = pl.multiple_of(c * CH, CH)
        m = mor[:, pl.ds(at, CH)]
        lo, hi = m & 255, m >> 8
        pick = hot(iota((256, CH), 0) == lo)
        wide = dot(tot, bas[:, pl.ds(at, CH)])
        leaf = jnp.broadcast_to(leaf_of(siz, at, CH), (16, CH))
        o = wide[0:16]
        for l in range(1, 32):
            o = jnp.where(leaf == l, wide[l * 16 : (l + 1) * 16], o)
        ob = o.astype(BF16)
        hib = jnp.broadcast_to(hi, (16, CH)).astype(F32).astype(BF16)
        for h in range(16):
            scat[h * 16 : (h + 1) * 16, :] = jnp.where(hib == h, ob, jnp.zeros((), BF16))
        return acc + dot(scat[...], pick, NT)

    acc = lax.fori_loop(0, 4096 // CH, chunk, jnp.zeros((256, 256), F32))
    for h in range(16):
        out[:, h * 256 : (h + 1) * 256] = acc[h * 16 : (h + 1) * 16]


S = jax.ShapeDtypeStruct
VM = pltpu.VMEM


def up(vec, mor, siz, bas, lt, mt, rt):
    return pl.pallas_call(up_kernel, out_shape=(S((512, 32), BF16), S((16, 32), BF16), S((16, 32), BF16)),
        scratch_shapes=[VM((512, 4096), BF16), VM((32, 1024), F32)])(vec, mor, siz, bas, lt, mt, rt)


def pairs_(idx, lc, coup):
    vm = pl.BlockSpec(memory_space=pltpu.VMEM)
    return pl.pallas_call(pair_kernel, out_shape=S((512, 32), F32),
        in_specs=[pl.BlockSpec(memory_space=pltpu.SMEM), vm, vm, vm],
        scratch_shapes=[VM((64, 1024), F32), VM((128, 32), BF16), VM((1024, 32), BF16), VM((1024, 32), BF16)])(idx, lc, idx, coup)


def down(top, far, mor, siz, bas, lt, mt):
    return pl.pallas_call(down_kernel, out_shape=S((16, 4096), F32),
        scratch_shapes=[VM((256, CH), BF16)])(top, far, mor, siz, bas, lt, mt)


highest = lax.Precision.HIGHEST


def from_everyone(array, axis):
    peers = lax.axis_size(axis)
    return lax.all_to_all(
        jnp.broadcast_to(array[None], (peers, *array.shape)), axis, 0, 0, tiled=True
    )


def in_order(parts, dim):
    dims = list(parts.shape[1:])
    dims[dim] *= parts.shape[0]
    return jnp.moveaxis(parts, 0, dim).reshape(dims)


def gathered_by_axis(array, axes, dim):
    far, near = axes
    parts = from_everyone(from_everyone(array, near), far)
    return in_order(parts.reshape(-1, *array.shape), dim)


def in_one_piece(arrays, axis, dim, along):
    ends, at = ([], 0)
    for a in arrays[:-1]:
        at += a.shape[along]
        ends.append(at)
    both = jnp.concatenate(arrays, axis=along)
    return tuple(jnp.split(gathered_by_axis(both, axis, dim), ends, axis=along))


def split_up(array, dim, peers):
    dims = array.shape
    parts = array.reshape(*dims[:dim], peers, dims[dim] // peers, *dims[dim + 1 :])
    return jnp.moveaxis(parts, dim, 0)


def sum_at_owner(array, axis, dim):
    peers = lax.axis_size(axis)
    parts = lax.all_to_all(split_up(array, dim, peers), axis, 0, 0, tiled=True)
    return jnp.sum(parts, axis=0)


def summed_rows(array, axes, dim):
    far, near = axes
    own = sum_at_owner(split_up(array, dim, lax.axis_size(far)), near, dim + 1)
    return jnp.sum(lax.all_to_all(own, far, 0, 0, tiled=True), axis=0)


def body(
    vectors,
    morton_order,
    leaf_sizes,
    leaf_basis,
    leaf_transfer,
    mid_transfer,
    root_transfer,
    leaf_pairs,
    leaf_coupling,
    dev_partner,
    dev_coupling,
    grp_partner,
    grp_coupling,
):
    basis_rank = leaf_basis.shape[0]
    count_vec = vectors.shape[0]
    row_width = basis_rank * count_vec
    subtrees = lax.axis_size(LEAF_AXES)
    groups = subtrees // 8
    self_id = lax.axis_index(LEAF_AXES)
    own_group = self_id // 8
    lc, root_t, term_t = up(
        vectors, morton_order, leaf_sizes, leaf_basis, leaf_transfer, mid_transfer, root_transfer
    )
    root_map = root_transfer.reshape(basis_rank, basis_rank)
    root_coeff = root_t.T
    group_term = term_t.T
    far = pairs_(leaf_pairs, lc, leaf_coupling)
    dev_blocks = dev_coupling.reshape(-1, basis_rank, basis_rank)
    partner = dev_partner[0]
    is_live = partner >= 0
    sent_back = jnp.einsum(
        "cij,iv->cjv", dev_blocks, root_coeff, preferred_element_type=jnp.float32
    ).reshape(-1, row_width)
    sent_back = jnp.where(is_live[:, None], sent_back, 0.0)
    every = jnp.arange(subtrees, dtype=jnp.int32)
    own_flat = root_coeff.reshape(1, row_width)
    term_flat = group_term.reshape(1, row_width)
    coeff_all, term_all = in_one_piece(
        (own_flat, term_flat), (("leaf_0", "leaf_1"), ("leaf_2", "leaf_3")), 0, 1
    )
    row_count = coeff_all.shape[0]
    here_ids = jnp.arange(row_count, dtype=jnp.int32)
    picker = (partner[:, None] == here_ids[None, :]).astype(jnp.bfloat16)
    chosen = jnp.dot(picker, coeff_all, preferred_element_type=jnp.float32).astype(jnp.bfloat16)
    chosen = chosen.reshape(-1, basis_rank, count_vec)
    near_sum = jnp.einsum("cij,cjv->iv", dev_blocks, chosen, preferred_element_type=jnp.float32)
    member = ((here_ids // 8)[None, :] == jnp.arange(groups, dtype=jnp.int32)[:, None]).astype(
        jnp.bfloat16
    )
    group_sum = jnp.dot(member, term_all, preferred_element_type=jnp.float32)
    near_sum, group_sum = (near_sum, group_sum)
    group_coeff = group_sum.astype(jnp.bfloat16)
    grp_blocks = grp_coupling.reshape(-1, basis_rank, basis_rank)
    group_hot = (grp_partner[0][:, None] == jnp.arange(groups, dtype=jnp.int32)[None, :]).astype(
        jnp.bfloat16
    )
    far_coeff = jnp.dot(group_hot, group_coeff, preferred_element_type=jnp.float32).astype(
        jnp.bfloat16
    )
    far_coeff = far_coeff.reshape(-1, basis_rank, count_vec)
    home_coeff = lax.dynamic_slice_in_dim(group_coeff, own_group, 1, 0).reshape(
        basis_rank, count_vec
    )
    to_own = jnp.einsum(
        "cij,cjv->iv", grp_blocks, far_coeff, preferred_element_type=jnp.float32
    ).reshape(1, row_width)
    to_far = jnp.einsum(
        "cij,iv->cjv", grp_blocks, home_coeff, preferred_element_type=jnp.float32
    ).reshape(-1, row_width)
    self_hot = (jnp.arange(groups, dtype=jnp.int32) == own_group).astype(jnp.float32)[:, None]
    group_rows = self_hot * to_own + jnp.dot(
        group_hot.astype(jnp.float32).T, to_far, precision=highest
    )
    partner_hot = (partner[:, None] == every[None, :]).astype(jnp.float32)
    dev_buffer = jnp.dot(partner_hot.T, sent_back, precision=highest)
    widened = jnp.concatenate([dev_buffer, jnp.repeat(group_rows, 8, axis=0)], axis=1)
    returns = summed_rows(widened, (("leaf_0", "leaf_1"), ("leaf_2", "leaf_3")), 0)
    dev_back = returns[:, :row_width]
    group_here = returns[:, row_width:]
    root_far = near_sum + dev_back.reshape(basis_rank, count_vec)
    group_far = group_here.reshape(basis_rank, count_vec).astype(jnp.bfloat16)
    from_group = jnp.dot(root_map, group_far, preferred_element_type=jnp.float32)
    root_total = (root_far + from_group).astype(jnp.bfloat16)
    return down(
        root_total.T, far, morton_order, leaf_sizes, leaf_basis, leaf_transfer, mid_transfer
    )


def solution(mesh):
    split = Mesh(mesh.devices.reshape(4, 8, 8, 2), ("leaf_0", "leaf_1", "leaf_2", "leaf_3"))
    in_specs = (
        P(None, LEAF_AXES),
        P(LEAF_AXES, None),
        P(LEAF_AXES, None),
        P(None, LEAF_AXES),
        P(LEAF_AXES, None),
        P(LEAF_AXES, None),
        P(LEAF_AXES, None),
        P(None, LEAF_AXES),
        P(LEAF_AXES, None),
        P(LEAF_AXES, None),
        P(LEAF_AXES, None),
        P(LEAF_AXES, None),
        P(LEAF_AXES, None),
    )
    out_specs = P(None, LEAF_AXES)
    return jax.shard_map(body, mesh=split, in_specs=in_specs, out_specs=out_specs, check_vma=False)
```

```python
import functools
import jax
import jax.numpy as jnp
from jax import lax
from jax.experimental import pallas as pl
from jax.experimental.pallas import tpu as pltpu
from jax.sharding import Mesh
from jax.sharding import PartitionSpec as P

F32, BF16, I32 = jnp.float32, jnp.bfloat16, jnp.int32
NT = (((1,), (1,)), ((), ()))
TN = (((0,), (0,)), ((), ()))


def iota(shape, dim):
    return lax.broadcasted_iota(I32, shape, dim)


def dot(a, b, dims=(((1,), (0,)), ((), ()))):
    return lax.dot_general(a, b, dims, preferred_element_type=F32)


def hot(mask):
    return jnp.where(mask, 1.0, 0.0).astype(BF16)


def spread_row():
    return hot(iota((32, 1024), 1) // 32 == iota((32, 1024), 0))


def spread_col():
    return hot(iota((32, 1024), 1) % 32 == iota((32, 1024), 0))


def fold_first(x):
    w = x[:, 0:128]
    for q in range(1, 8):
        w = w + x[:, q * 128 : (q + 1) * 128]
    return (w[:, 0:32] + w[:, 32:64]) + (w[:, 64:96] + w[:, 96:128])


def leaf_of(siz_ref, start, width):
    sizes = siz_ref[...].astype(F32)
    lower = iota((32, 32), 1) <= iota((32, 32), 0)
    ends = jnp.sum(jnp.where(lower, jnp.broadcast_to(sizes, (32, 32)), 0.0), axis=1, keepdims=True)
    pos = (iota((32, width), 1) + start).astype(F32)
    return jnp.sum(jnp.where(pos >= ends, 1.0, 0.0), axis=0, keepdims=True)


CH = 256


def up_kernel(vec, mor, siz, bas, lt, mt, rt, lc_out, root_out, term_out, masked, lt32):
    lt32[...] = lt[...].astype(F32)
    vx = jnp.concatenate([vec[:, h * 256 : (h + 1) * 256] for h in range(16)], axis=0).astype(BF16)

    def chunk(c, carry):
        at = pl.multiple_of(c * CH, CH)
        m = mor[:, pl.ds(at, CH)]
        lo, hi = m & 255, m >> 8
        pick = hot(iota((256, CH), 0) == lo)
        wide = dot(vx, pick)
        hib = jnp.broadcast_to(hi, (16, CH))
        sv = wide[0:16]
        for h in range(1, 16):
            sv = jnp.where(hib == h, wide[h * 16 : (h + 1) * 16], sv)
        leaf = jnp.broadcast_to(leaf_of(siz, at, CH), (16, CH)).astype(BF16)
        svb = sv.astype(BF16)
        for l in range(32):
            masked[l * 16 : (l + 1) * 16, pl.ds(at, CH)] = jnp.where(leaf == l, svb, jnp.zeros((), BF16))
        return carry

    lax.fori_loop(0, 4096 // CH, chunk, 0)
    lc = dot(masked[...], bas[...], NT).astype(BF16)
    lc_out[...] = lc
    erow = spread_row()
    root = jnp.zeros((16, 1024), F32)
    for m in range(4):
        acc = jnp.zeros((16, 1024), F32)
        x = dot(lc[m * 128 : (m + 1) * 128], erow)
        for l in range(8):
            acc = acc + x[l * 16 : (l + 1) * 16] * lt32[m * 8 + l : m * 8 + l + 1, :]
        mid = fold_first(acc).astype(BF16)
        root = root + dot(mid, erow) * mt[m : m + 1, :].astype(F32)
    root = fold_first(root).astype(BF16)
    root_out[...] = root
    term_out[...] = fold_first(dot(root, erow) * rt[...].astype(F32)).astype(BF16)


def pair_kernel(idx, lc, pairs, coup, far_out, s32, got, fwd, bwd):
    s32[...] = coup[...].astype(F32)
    erow, ecol = spread_row(), spread_col()
    back = hot(iota((1024, 32), 0) // 32 == iota((1024, 32), 1))

    def group(g, carry):
        for which, e in ((1, ecol), (0, erow)):
            for k in range(8):
                b = idx[which, g * 8 + k]
                got[k * 16 : (k + 1) * 16, :] = lc[pl.ds(pl.multiple_of(b * 16, 16), 16), :]
            x = dot(got[...], e)
            parts = [x[k * 16 : (k + 1) * 16] * s32[pl.ds(g * 8 + k, 1), :] for k in range(8)]
            if which == 1:
                y = dot(jnp.concatenate(parts, axis=0).astype(BF16), back)
                fwd[pl.ds(pl.multiple_of(g * 128, 128), 128), :] = y.astype(BF16)
            else:
                y = jnp.concatenate([fold_first(t) for t in parts], axis=0)
                bwd[pl.ds(pl.multiple_of(g * 128, 128), 128), :] = y.astype(BF16)
        return carry

    lax.fori_loop(0, 8, group, 0)
    wide = hot(iota((64, 1024), 1) // 16 == iota((64, 1024), 0))
    ids = dot(pairs[...].astype(F32).astype(BF16), wide)
    same = iota((512, 1024), 0) % 16 == iota((512, 1024), 1) % 16
    leaf = (iota((512, 1024), 0) // 16).astype(F32)
    far_out[...] = dot(hot(same & (leaf == ids[0:1])), fwd[...]) + dot(hot(same & (leaf == ids[1:2])), bwd[...])


def down_kernel(top, far, mor, siz, bas, lt, mt, out, scat):
    erow, ecol = spread_row(), spread_col()
    back = hot(iota((1024, 32), 0) // 32 == iota((1024, 32), 1))
    xt = dot(top[...], ecol)
    p = jnp.concatenate([xt * mt[m : m + 1, :].astype(F32) for m in range(4)], axis=0)
    ph = p.astype(BF16)
    pl_ = (p - ph.astype(F32)).astype(BF16)
    mid = (dot(ph, back) + dot(pl_, back)).astype(BF16)
    tots = []
    for m in range(4):
        x = dot(mid[m * 16 : (m + 1) * 16], ecol)
        q = jnp.concatenate(
            [x * lt[m * 8 + l : m * 8 + l + 1, :].astype(F32) for l in range(8)], axis=0
        ).astype(BF16)
        tots.append((dot(q, back) + far[m * 128 : (m + 1) * 128, :]).astype(BF16))
    tot = jnp.concatenate(tots, axis=0)

    def chunk(c, acc):
        at = pl.multiple_of(c * CH, CH)
        m = mor[:, pl.ds(at, CH)]
        lo, hi = m & 255, m >> 8
        pick = hot(iota((256, CH), 0) == lo)
        wide = dot(tot, bas[:, pl.ds(at, CH)])
        leaf = jnp.broadcast_to(leaf_of(siz, at, CH), (16, CH))
        o = wide[0:16]
        for l in range(1, 32):
            o = jnp.where(leaf == l, wide[l * 16 : (l + 1) * 16], o)
        ob = o.astype(BF16)
        hib = jnp.broadcast_to(hi, (16, CH)).astype(F32).astype(BF16)
        for h in range(16):
            scat[h * 16 : (h + 1) * 16, :] = jnp.where(hib == h, ob, jnp.zeros((), BF16))
        return acc + dot(scat[...], pick, NT)

    acc = lax.fori_loop(0, 4096 // CH, chunk, jnp.zeros((256, 256), F32))
    for h in range(16):
        out[:, h * 256 : (h + 1) * 256] = acc[h * 16 : (h + 1) * 16]


S = jax.ShapeDtypeStruct
VM = pltpu.VMEM


def up(vec, mor, siz, bas, lt, mt, rt):
    return pl.pallas_call(up_kernel, out_shape=(S((512, 32), BF16), S((16, 32), BF16), S((16, 32), BF16)),
        scratch_shapes=[VM((512, 4096), BF16), VM((32, 1024), F32)])(vec, mor, siz, bas, lt, mt, rt)


def pairs_(idx, lc, coup):
    vm = pl.BlockSpec(memory_space=pltpu.VMEM)
    return pl.pallas_call(pair_kernel, out_shape=S((512, 32), F32),
        in_specs=[pl.BlockSpec(memory_space=pltpu.SMEM), vm, vm, vm],
        scratch_shapes=[VM((64, 1024), F32), VM((128, 32), BF16), VM((1024, 32), BF16), VM((1024, 32), BF16)])(idx, lc, idx, coup)


def down(top, far, mor, siz, bas, lt, mt):
    return pl.pallas_call(down_kernel, out_shape=S((16, 4096), F32),
        scratch_shapes=[VM((256, CH), BF16)])(top, far, mor, siz, bas, lt, mt)


AXES = ("leaf_0", "leaf_1", "leaf_2", "leaf_3")
MESH = pl.DeviceIdType.MESH


def split2(x):
    hi = x.astype(BF16)
    return hi, (x - hi.astype(F32)).astype(BF16)


def pack_row(c):
    wide = dot(c, hot(iota((32, 128), 1) % 32 == iota((32, 128), 0)))
    wide = jnp.where(iota((16, 128), 1) // 32 == iota((16, 128), 0) % 4, wide, 0.0).astype(BF16)
    return dot(hot(iota((4, 16), 1) // 4 == iota((4, 16), 0)), wide)


def unpack_row(r):
    sel = hot(iota((16, 4), 0) // 4 == iota((16, 4), 1))
    hi, lo = split2(r)
    wide = dot(sel, hi) + dot(sel, lo)
    wide = jnp.where(iota((16, 128), 1) // 32 == iota((16, 128), 0) % 4, wide, 0.0)
    return (wide[:, 0:32] + wide[:, 32:64]) + (wide[:, 64:96] + wide[:, 96:128])


def sum_rows(ref, n):
    flat = ref[...].reshape(n * 4, 128)
    return dot(hot(iota((4, n * 4), 1) % 4 == iota((4, n * 4), 0)), flat)


def back_weights(c, w):
    cex = dot(c, hot(iota((16, 512), 1) // 32 == iota((16, 512), 0)), TN)
    same = iota((32, 512), 1) % 32 == iota((32, 512), 0)
    for i in range(32):
        row = jnp.broadcast_to(cex[i : i + 1, :], (32, 512))
        w[i * 32 : (i + 1) * 32, :] = jnp.where(same, row, 0.0).astype(BF16)


def forward_sum(blocks, chosen):
    same = iota((32, 512), 1) % 32 == iota((32, 512), 0)
    rows = []
    for q in range(4):
        part = dot(blocks[:, q * 256 : (q + 1) * 256], chosen, TN)
        for i in range(8):
            rows.append(jnp.sum(jnp.where(same, part[i * 32 : (i + 1) * 32], 0.0), axis=0, keepdims=True))
    y = jnp.concatenate(rows, axis=0)
    hi, lo = split2(y)
    sel = hot(iota((16, 512), 1) // 32 == iota((16, 512), 0))
    return dot(sel, hi, NT) + dot(sel, lo, NT)


def lanes_of(ref, n):
    return jnp.concatenate([ref[:, q, :] for q in range(4)], axis=1)


def comm_kernel(dims, root_ref, term_ref, partner, dcoup, gpart, gcoup, rt, top_out,
                ca, rsb, rx, sb, rr, gx, sgx, pgx, gcb, tb, gr, w, rowb, termb, pgs, gcrow,
                send, recv):
    nx, ny, nz = dims
    chips = nx * ny * nz
    groups = chips // 4
    x, y, z, c = [lax.axis_index(a) for a in AXES]
    chip = (x * ny + y) * nz + z
    g = chip // 4
    zq = z % 4
    k = zq * 2 + c

    def at_chip(d):
        dx = d // (ny * nz) + nx // 2
        dy = (d // nz) % ny + ny // 2
        dz = d % nz + nz // 2
        return (x + dx) % nx, (y + dy) % ny, (z + dz) % nz

    own = ((nx - nx // 2) % nx * ny + (ny - ny // 2) % ny) * nz + (nz - nz // 2) % nz

    def every_chip(f):
        lax.fori_loop(0, own, lambda d, s: (f(*at_chip(d)), s)[1], 0)
        lax.fori_loop(own + 1, chips, lambda d, s: (f(*at_chip(d)), s)[1], 0)

    def mate(j):
        r = (k + j) % 8
        return (x, y, z - zq + r // 2, r % 2)

    halves = nz // 4

    def group_peer(d):
        h = (g + d) % groups
        return h, (h // (ny * halves), (h // halves) % ny, (h % halves) * 4 + zq, c)

    def every_group(f):
        lax.fori_loop(1, groups, lambda d, s: (f(*group_peer(d)), s)[1], 0)

    sibling = (x, y, z, 1 - c)

    def push(src, dst, i, to):
        pltpu.make_async_remote_copy(src, dst, send.at[i], recv.at[i], device_id=to, device_id_type=MESH).start()

    def await_(src, dst, i, to, which):
        cp = pltpu.make_async_remote_copy(src, dst, send.at[i], recv.at[i], device_id=to, device_id_type=MESH)
        (cp.wait_recv if which else cp.wait_send)()

    def got(ref, i):
        await_(ref, ref, i, sibling, True)

    def sent(ref, i):
        await_(ref, ref, i, sibling, False)

    bar = pltpu.get_barrier_semaphore()

    def greet(to):
        pl.semaphore_signal(bar, inc=1, device_id=to, device_id_type=MESH)

    every_chip(lambda a, b, d: greet((a, b, d, c)))
    others = 0
    for j in range(1, 8):
        r = (k + j) % 8

        @pl.when(r % 2 != c)
        def _():
            greet(mate(j))

    pgs[...] = jnp.zeros((1, 128), I32)
    pgs[:, 0:4] = gpart[...]
    rowb[...] = pack_row(root_ref[...]).astype(BF16)
    termb[...] = pack_row(term_ref[...]).astype(BF16)
    pl.semaphore_wait(bar, chips - 1 + 4)

    for j in range(1, 8):
        push(termb, gx.at[k], 0, mate(j))
    for j in range(1, 8):
        push(gcoup, sgx.at[k], 1, mate(j))
        push(pgs, pgx.at[k], 2, mate(j))
    every_chip(lambda a, b, d: push(rowb, ca.at[c, chip], 3, (a, b, d, c)))
    gx[k] = termb[...]
    sgx[k] = gcoup[...]
    pgx[k] = pgs[...]
    ca[c, chip] = rowb[...]

    back_weights(root_ref[...], w)
    bk = dot(dcoup[...], w[...]).astype(BF16)
    for half in range(2):
        ids = iota((chips, 128), 0) * 2 + half
        hotb = hot(ids == jnp.broadcast_to(partner[...], (chips, 128)))
        r = dot(hotb, bk).astype(BF16)
        for q in range(4):
            rsb[half, :, q, :] = r[:, q * 128 : (q + 1) * 128]
    push(rsb.at[1 - c], rx, 4, sibling)

    got(gx.at[pl.ds(0, 7)], 0)
    gcoef = sum_rows(gx, 8).astype(BF16)
    gcrow[...] = gcoef
    every_group(lambda h, to: push(gcrow, gcb.at[g], 5, to))
    gcb[g] = gcoef

    got(rx, 4)
    sb[...] = (rsb[c].astype(F32) + rx[...].astype(F32)).astype(BF16)

    def send_back(a, b, d):
        push(sb.at[(a * ny + b) * nz + d], rr.at[chip], 6, (a, b, d, c))

    every_chip(send_back)
    rr[chip] = sb[chip]

    got(sgx.at[pl.ds(0, 7)], 1)
    got(pgx.at[pl.ds(0, 7)], 2)
    sg = sgx[...].reshape(32, 1024)
    p8 = pgx[...].reshape(8, 128).astype(F32).astype(BF16)[:, 0:4]
    spread = dot(p8, hot(iota((4, 32), 1) % 4 == iota((4, 32), 0)))
    pair = jnp.sum(jnp.where(iota((8, 32), 1) // 4 == iota((8, 32), 0), spread, 0.0), axis=0, keepdims=True)
    hotg = hot(iota((groups, 32), 0).astype(F32) == jnp.broadcast_to(pair, (groups, 32)))
    back_weights(unpack_row(gcoef.astype(F32)).astype(BF16), w)
    t = dot(hotg, dot(sg, w[...]).astype(BF16)).astype(BF16)
    for q in range(4):
        tb[:, q, :] = t[:, q * 128 : (q + 1) * 128]
    every_group(lambda h, to: push(tb.at[h], gr.at[g], 7, to))
    gr[g] = tb[g]

    got(ca.at[0, pl.ds(0, chips - 1)], 3)
    push(ca.at[c], ca.at[c], 8, sibling)
    got(ca.at[0], 8)
    near = jnp.zeros((128, 512), F32)
    for half in range(2):
        ids = iota((chips, 128), 0) * 2 + half
        hotb = hot(ids == jnp.broadcast_to(partner[...], (chips, 128)))
        near = near + dot(hotb, lanes_of(ca.at[half], chips), TN)
    root_far = forward_sum(dcoup[...], near.astype(BF16))
    got(gcb.at[pl.ds(0, groups - 1)], 5)
    far = dot(hotg, lanes_of(gcb, groups), TN).astype(BF16)
    group_far = forward_sum(sg, far)

    got(rr.at[pl.ds(0, chips - 1)], 6)
    root_far = root_far + unpack_row(sum_rows(rr, chips))
    got(gr.at[pl.ds(0, groups - 1)], 7)
    group_far = (group_far + unpack_row(sum_rows(gr, groups))).astype(BF16)
    ecol = spread_col()
    back = hot(iota((1024, 32), 0) // 32 == iota((1024, 32), 1))
    hi, lo = split2(dot(group_far, ecol) * rt[...].astype(F32))
    top_out[...] = (root_far + dot(hi, back) + dot(lo, back)).astype(BF16)

    sent(gx.at[pl.ds(0, 7)], 0)
    sent(sgx.at[pl.ds(0, 7)], 1)
    sent(pgx.at[pl.ds(0, 7)], 2)
    sent(ca.at[0, pl.ds(0, chips - 1)], 3)
    sent(rx, 4)
    sent(gcb.at[pl.ds(0, groups - 1)], 5)
    sent(rr.at[pl.ds(0, chips - 1)], 6)
    sent(gr.at[pl.ds(0, groups - 1)], 7)
    sent(ca.at[0], 8)


def comm_scratch(chips):
    groups = chips // 4
    b = lambda *s: pltpu.VMEM(s, BF16)
    return [b(2, chips, 4, 128), b(2, chips, 4, 128), b(chips, 4, 128), b(chips, 4, 128), b(chips, 4, 128),
            b(8, 4, 128), b(8, 4, 1024), pltpu.VMEM((8, 1, 128), I32), b(groups, 4, 128), b(groups, 4, 128),
            b(groups, 4, 128), b(1024, 512), b(4, 128), b(4, 128), pltpu.VMEM((1, 128), I32), b(4, 128),
            pltpu.SemaphoreType.DMA((9,)), pltpu.SemaphoreType.DMA((9,))]


def comm(dims, root, term, partner, dcoup, gpart, gcoup, rt):
    chips = dims[0] * dims[1] * dims[2]
    return pl.pallas_call(functools.partial(comm_kernel, dims), out_shape=jax.ShapeDtypeStruct((16, 32), BF16),
        scratch_shapes=comm_scratch(chips),
        compiler_params=pltpu.CompilerParams(collective_id=0, has_side_effects=True))(
            root, term, partner, dcoup, gpart, gcoup, rt)


def body(dims, vec, mor, siz, bas, lt, mt, rt, pairs, lcoup, partner, dcoup, gpart, gcoup):
    lc, root, term = up(vec, mor, siz, bas, lt, mt, rt)
    top = comm(dims, root, term, partner, dcoup, gpart, gcoup, rt)
    far = pairs_(pairs, lc, lcoup)
    return down(top, far, mor, siz, bas, lt, mt)


def solution(mesh):
    split = Mesh(mesh.devices.reshape(4, 8, 8, 2), AXES)
    rows, cols = P(AXES, None), P(None, AXES)
    in_specs = (cols, rows, rows, cols, rows, rows, rows, cols, rows, rows, rows, rows, rows)
    step = functools.partial(body, (4, 8, 8))
    return jax.shard_map(step, mesh=split, in_specs=in_specs, out_specs=cols, check_vma=False)
```

```python
import functools
import jax
import jax.numpy as jnp
from jax import lax
from jax.experimental import pallas as pl
from jax.experimental.pallas import tpu as pltpu
from jax.sharding import Mesh
from jax.sharding import PartitionSpec as P

F32, BF16, I32 = jnp.float32, jnp.bfloat16, jnp.int32
NT = (((1,), (1,)), ((), ()))
TN = (((0,), (0,)), ((), ()))


def iota(shape, dim):
    return lax.broadcasted_iota(I32, shape, dim)


def dot(a, b, dims=(((1,), (0,)), ((), ()))):
    return lax.dot_general(a, b, dims, preferred_element_type=F32)


def hot(mask):
    return jnp.where(mask, 1.0, 0.0).astype(BF16)


def spread_row():
    return hot(iota((32, 1024), 1) // 32 == iota((32, 1024), 0))


def spread_col():
    return hot(iota((32, 1024), 1) % 32 == iota((32, 1024), 0))


def fold_first(x):
    w = x[:, 0:128]
    for q in range(1, 8):
        w = w + x[:, q * 128 : (q + 1) * 128]
    return (w[:, 0:32] + w[:, 32:64]) + (w[:, 64:96] + w[:, 96:128])


def leaf_of(siz_ref, start, width):
    sizes = siz_ref[...].astype(F32)
    lower = iota((32, 32), 1) <= iota((32, 32), 0)
    ends = jnp.sum(jnp.where(lower, jnp.broadcast_to(sizes, (32, 32)), 0.0), axis=1, keepdims=True)
    pos = (iota((32, width), 1) + start).astype(F32)
    return jnp.sum(jnp.where(pos >= ends, 1.0, 0.0), axis=0, keepdims=True)


CH = 256


def down_kernel(top, far, mor, siz, bas, lt, mt, out, scat):
    erow, ecol = spread_row(), spread_col()
    back = hot(iota((1024, 32), 0) // 32 == iota((1024, 32), 1))
    xt = dot(top[...], ecol)
    p = jnp.concatenate([xt * mt[m : m + 1, :].astype(F32) for m in range(4)], axis=0)
    ph = p.astype(BF16)
    pl_ = (p - ph.astype(F32)).astype(BF16)
    mid = (dot(ph, back) + dot(pl_, back)).astype(BF16)
    tots = []
    for m in range(4):
        x = dot(mid[m * 16 : (m + 1) * 16], ecol)
        q = jnp.concatenate(
            [x * lt[m * 8 + l : m * 8 + l + 1, :].astype(F32) for l in range(8)], axis=0
        ).astype(BF16)
        tots.append((dot(q, back) + far[m * 128 : (m + 1) * 128, :]).astype(BF16))
    tot = jnp.concatenate(tots, axis=0)

    def chunk(c, acc):
        at = pl.multiple_of(c * CH, CH)
        m = mor[:, pl.ds(at, CH)]
        lo, hi = m & 255, m >> 8
        pick = hot(iota((256, CH), 0) == lo)
        wide = dot(tot, bas[:, pl.ds(at, CH)])
        leaf = jnp.broadcast_to(leaf_of(siz, at, CH), (16, CH))
        o = wide[0:16]
        for l in range(1, 32):
            o = jnp.where(leaf == l, wide[l * 16 : (l + 1) * 16], o)
        ob = o.astype(BF16)
        hib = jnp.broadcast_to(hi, (16, CH)).astype(F32).astype(BF16)
        for h in range(16):
            scat[h * 16 : (h + 1) * 16, :] = jnp.where(hib == h, ob, jnp.zeros((), BF16))
        return acc + dot(scat[...], pick, NT)

    acc = lax.fori_loop(0, 4096 // CH, chunk, jnp.zeros((256, 256), F32))
    for h in range(16):
        out[:, h * 256 : (h + 1) * 256] = acc[h * 16 : (h + 1) * 16]


S = jax.ShapeDtypeStruct
VM = pltpu.VMEM


def down(top, far, mor, siz, bas, lt, mt):
    return pl.pallas_call(down_kernel, out_shape=S((16, 4096), F32),
        scratch_shapes=[VM((256, CH), BF16)])(top, far, mor, siz, bas, lt, mt)


AXES = ("leaf_0", "leaf_1", "leaf_2", "leaf_3")
MESH = pl.DeviceIdType.MESH


def split2(x):
    hi = x.astype(BF16)
    return hi, (x - hi.astype(F32)).astype(BF16)


def pack_row(c):
    wide = dot(c, hot(iota((32, 128), 1) % 32 == iota((32, 128), 0)))
    wide = jnp.where(iota((16, 128), 1) // 32 == iota((16, 128), 0) % 4, wide, 0.0).astype(BF16)
    return dot(hot(iota((4, 16), 1) // 4 == iota((4, 16), 0)), wide)


def unpack_row(r):
    sel = hot(iota((16, 4), 0) // 4 == iota((16, 4), 1))
    hi, lo = split2(r)
    wide = dot(sel, hi) + dot(sel, lo)
    wide = jnp.where(iota((16, 128), 1) // 32 == iota((16, 128), 0) % 4, wide, 0.0)
    return (wide[:, 0:32] + wide[:, 32:64]) + (wide[:, 64:96] + wide[:, 96:128])


def sum_rows(ref, n):
    flat = ref[...].reshape(n * 4, 128)
    return dot(hot(iota((4, n * 4), 1) % 4 == iota((4, n * 4), 0)), flat)


def back_weights(c, w):
    cex = dot(c, hot(iota((16, 512), 1) // 32 == iota((16, 512), 0)), TN)
    same = iota((32, 512), 1) % 32 == iota((32, 512), 0)
    for i in range(32):
        row = jnp.broadcast_to(cex[i : i + 1, :], (32, 512))
        w[i * 32 : (i + 1) * 32, :] = jnp.where(same, row, 0.0).astype(BF16)


def forward_sum(blocks, chosen):
    same = iota((32, 512), 1) % 32 == iota((32, 512), 0)
    rows = []
    for q in range(4):
        part = dot(blocks[:, q * 256 : (q + 1) * 256], chosen, TN)
        for i in range(8):
            rows.append(jnp.sum(jnp.where(same, part[i * 32 : (i + 1) * 32], 0.0), axis=0, keepdims=True))
    y = jnp.concatenate(rows, axis=0)
    hi, lo = split2(y)
    sel = hot(iota((16, 512), 1) // 32 == iota((16, 512), 0))
    return dot(sel, hi, NT) + dot(sel, lo, NT)


def lanes_of(x):
    return x.reshape(x.shape[0], 512)


def add_all(terms):
    return functools.reduce(lambda a, b: a + b, [t.astype(F32) for t in terms]).astype(BF16)


def mega_kernel(dims, vec, mor, siz, bas, lt, mt, rt, pairs, lcoup, partner, dcoup, gpart, gcoup,
                top_out, far_out,
                masked, lt32, lc, s32, idcol, fwd, bwd,
                ca, rsb, rx, sb, rx2, sb2, rr, gx, sgx, pgx, gcb, tb, gr2, tb2, gr, w,
                rowb, termb, pgs, gcrow, send, recv):
    nx, ny, nz = dims
    halves = nz // 4
    plane, pgs_n = ny * nz, ny * halves
    x, y, z, c = [lax.axis_index(a) for a in AXES]
    zq, zh = z % 4, z // 4
    k = zq * 2 + c
    yz = y * nz + z
    pg = y * halves + zh
    xs = [(x + j) % nx for j in range(nx)]
    ys = [(y + j) % ny for j in range(ny)]
    zs = [(z + j) % nz for j in range(nz)]
    gz = [((zh + j) % halves) * 4 + zq for j in range(halves)]
    far_first = lambda o: -(min(o[0], ny - o[0]) + min(o[1], nz - o[1]))
    offs = sorted([(a, b) for a in range(ny) for b in range(nz) if a or b], key=far_first)
    goffs = sorted([(a, b) for a in range(ny) for b in range(halves) if a or b], key=lambda o: -min(o[0], ny - o[0]))
    sibling = (x, y, z, 1 - c)

    def mate(j):
        r = (k + j) % 8
        return (x, y, zh * 4 + r // 2, r % 2)

    def push(src, dst, i, to):
        pltpu.make_async_remote_copy(src, dst, send.at[i], recv.at[i], device_id=to, device_id_type=MESH).start()

    def settle(ref, i, which):
        cp = pltpu.make_async_remote_copy(
            ref, ref, send.at[i], recv.at[i], device_id=sibling, device_id_type=MESH
        )
        (cp.wait_recv if which else cp.wait_send)()

    def got(ref, i):
        settle(ref, i, True)

    def sent(ref, i):
        settle(ref, i, False)

    bar = pltpu.get_barrier_semaphore()

    def greet(to):
        pl.semaphore_signal(bar, inc=1, device_id=to, device_id_type=MESH)

    for a, b in offs:
        greet((x, ys[a], zs[b], c))
    for j in range(1, nx):
        greet((xs[j], y, z, c))
    for j in range(1, 8):

        @pl.when((k + j) % 2 != c)
        def _():
            greet(mate(j))

    pgs[...] = jnp.zeros((1, 128), I32)
    pgs[:, 0:4] = gpart[...]
    lt32[...] = lt[...].astype(F32)
    vx = jnp.concatenate([vec[:, h * 256 : (h + 1) * 256] for h in range(16)], axis=0).astype(BF16)

    def chunk(i, carry):
        at = pl.multiple_of(i * CH, CH)
        m = mor[:, pl.ds(at, CH)]
        lo, hi = m & 255, m >> 8
        wide = dot(vx, hot(iota((256, CH), 0) == lo))
        hib = jnp.broadcast_to(hi, (16, CH))
        sv = wide[0:16]
        for h in range(1, 16):
            sv = jnp.where(hib == h, wide[h * 16 : (h + 1) * 16], sv)
        leaf = jnp.broadcast_to(leaf_of(siz, at, CH), (16, CH)).astype(BF16)
        svb = sv.astype(BF16)
        for l in range(32):
            masked[l * 16 : (l + 1) * 16, pl.ds(at, CH)] = jnp.where(leaf == l, svb, jnp.zeros((), BF16))
        return carry

    lax.fori_loop(0, 4096 // CH, chunk, 0)
    lcv = dot(masked[...], bas[...], NT).astype(BF16)
    lc[...] = lcv
    erow, ecol = spread_row(), spread_col()
    root = jnp.zeros((16, 1024), F32)
    for m in range(4):
        acc = jnp.zeros((16, 1024), F32)
        wide = dot(lcv[m * 128 : (m + 1) * 128], erow)
        for l in range(8):
            acc = acc + wide[l * 16 : (l + 1) * 16] * lt32[m * 8 + l : m * 8 + l + 1, :]
        mid = fold_first(acc).astype(BF16)
        root = root + dot(mid, erow) * mt[m : m + 1, :].astype(F32)
    root = fold_first(root).astype(BF16)
    term = fold_first(dot(root, erow) * rt[...].astype(F32)).astype(BF16)
    termb[...] = pack_row(term).astype(BF16)
    rowb[...] = pack_row(root).astype(BF16)
    pl.semaphore_wait(bar, plane - 1 + nx - 1 + 4)

    for j in range(1, 8):
        push(termb, gx.at[k], 0, mate(j))
    for a, b in offs:
        push(rowb, ca.at[c, x, yz], 3, (x, ys[a], zs[b], c))
    for j in range(1, 8):
        push(gcoup, sgx.at[k], 1, mate(j))
        push(pgs, pgx.at[k], 2, mate(j))
    gx[k] = termb[...]
    sgx[k] = gcoup[...]
    pgx[k] = pgs[...]
    ca[c, x, yz] = rowb[...]

    back_weights(root, w)
    bk = dot(dcoup[...], w[...]).astype(BF16)
    chips = nx * plane
    for half in range(2):
        ids = iota((chips, 128), 0) * 2 + half
        hotb = hot(ids == jnp.broadcast_to(partner[...], (chips, 128)))
        rsb[half] = dot(hotb, bk).astype(BF16).reshape(nx, plane, 4, 128)
    push(rsb.at[1 - c], rx, 4, sibling)

    got(gx.at[pl.ds(0, 7)], 0)
    gcoef = sum_rows(gx, 8).astype(BF16)
    gcrow[...] = gcoef
    for a, b in goffs:
        push(gcrow, gcb.at[x, pg], 5, (x, ys[a], gz[b], c))
    gcb[x, pg] = gcoef

    got(sgx.at[pl.ds(0, 7)], 1)
    got(pgx.at[pl.ds(0, 7)], 2)
    sg = sgx[...].reshape(32, 1024)
    groups = nx * pgs_n
    p8 = pgx[...].reshape(8, 128).astype(F32).astype(BF16)[:, 0:4]
    spread = dot(p8, hot(iota((4, 32), 1) % 4 == iota((4, 32), 0)))
    gpair = jnp.sum(jnp.where(iota((8, 32), 1) // 4 == iota((8, 32), 0), spread, 0.0), axis=0, keepdims=True)
    hotg = hot(iota((groups, 32), 0).astype(F32) == jnp.broadcast_to(gpair, (groups, 32)))
    back_weights(unpack_row(gcoef.astype(F32)).astype(BF16), w)
    tb[...] = dot(hotg, dot(sg, w[...]).astype(BF16)).astype(BF16).reshape(nx, pgs_n, 4, 128)
    for j in range(1, nx):
        push(tb.at[xs[j]], gr2.at[j - 1], 7, (xs[j], y, z, c))

    got(rx, 4)
    sb[...] = add_all([rsb[c], rx[...]])
    for j in range(1, nx):
        push(sb.at[xs[j]], rx2.at[j - 1], 6, (xs[j], y, z, c))

    s32[...] = lcoup[...].astype(F32)
    each = hot(iota((64, 1024), 1) // 16 == iota((64, 1024), 0))
    pairsb = pairs[...].astype(F32).astype(BF16)
    idcol[...] = dot(each, pairsb, (((0,), (1,)), ((), ())))
    back = hot(iota((1024, 32), 0) // 32 == iota((1024, 32), 1))

    def leaf_group(gi, carry):
        at = pl.multiple_of(gi * 128, 128)
        eye = iota((128, 512), 0) % 16 == iota((128, 512), 1) % 16
        for which, e in ((1, ecol), (0, erow)):
            leaf = jnp.broadcast_to(idcol[pl.ds(at, 128), which : which + 1], (128, 512))
            chosen = dot(hot(eye & (leaf == (iota((128, 512), 1) // 16).astype(F32))), lc[...]).astype(BF16)
            wide = dot(chosen, e)
            parts = [wide[t * 16 : (t + 1) * 16] * s32[pl.ds(gi * 8 + t, 1), :] for t in range(8)]
            if which == 1:
                out = dot(jnp.concatenate(parts, axis=0).astype(BF16), back)
                fwd[pl.ds(at, 128), :] = out.astype(BF16)
            else:
                out = jnp.concatenate([fold_first(t) for t in parts], axis=0)
                bwd[pl.ds(at, 128), :] = out.astype(BF16)
        return carry

    lax.fori_loop(0, 3, leaf_group, 0)

    got(ca.at[c, x, pl.ds(0, plane - 1)], 3)
    for j in range(1, nx):
        push(ca.at[c, x], ca.at[c, x], 9, (xs[j], y, z, c))
    push(ca.at[c, x], ca.at[c, x], 8, sibling)

    got(rx2, 6)
    sb2[...] = add_all([sb[x]] + [rx2[j] for j in range(nx - 1)])
    for a, b in offs:
        push(sb2.at[ys[a] * nz + zs[b]], rr.at[yz], 10, (x, ys[a], zs[b], c))
    rr[yz] = sb2[yz]
    got(gr2, 7)
    tb2[...] = add_all([tb[x]] + [gr2[j] for j in range(nx - 1)])
    for a, b in goffs:
        push(tb2.at[ys[a] * halves + (zh + b) % halves], gr.at[pg], 11, (x, ys[a], gz[b], c))
    gr[pg] = tb2[pg]

    got(gcb.at[x, pl.ds(0, pgs_n - 1)], 5)
    for j in range(1, nx):
        push(gcb.at[x], gcb.at[x], 12, (xs[j], y, z, c))

    lax.fori_loop(3, 8, leaf_group, 0)

    got(ca.at[c, pl.ds(0, nx - 1)], 9)
    for j in range(1, nx):
        push(ca.at[c, xs[j]], ca.at[c, xs[j]], 13, sibling)
    ids = dot(pairsb, each)
    same = iota((512, 1024), 0) % 16 == iota((512, 1024), 1) % 16
    leaf = (iota((512, 1024), 0) // 16).astype(F32)
    far_out[...] = dot(hot(same & (leaf == ids[0:1])), fwd[...]) + dot(hot(same & (leaf == ids[1:2])), bwd[...])
    got(ca.at[c, x], 8)
    got(ca.at[c, pl.ds(0, nx - 1)], 13)
    near = jnp.zeros((128, 512), F32)
    for half in range(2):
        ids = iota((chips, 128), 0) * 2 + half
        hotb = hot(ids == jnp.broadcast_to(partner[...], (chips, 128)))
        near = near + dot(hotb, lanes_of(ca[half].reshape(chips, 4, 128)), TN)
    root_far = forward_sum(dcoup[...], near.astype(BF16))
    got(gcb.at[pl.ds(0, nx - 1)], 12)
    far = dot(hotg, lanes_of(gcb[...].reshape(groups, 4, 128)), TN).astype(BF16)
    group_far = forward_sum(sg, far)

    got(rr.at[pl.ds(0, plane - 1)], 10)
    root_far = root_far + unpack_row(sum_rows(rr, plane))
    got(gr.at[pl.ds(0, pgs_n - 1)], 11)
    group_far = (group_far + unpack_row(sum_rows(gr, pgs_n))).astype(BF16)
    hi, lo = split2(dot(group_far, ecol) * rt[...].astype(F32))
    top_out[...] = (root_far + dot(hi, back) + dot(lo, back)).astype(BF16)

    sent(gx.at[pl.ds(0, 7)], 0)
    sent(sgx.at[pl.ds(0, 7)], 1)
    sent(pgx.at[pl.ds(0, 7)], 2)
    sent(ca.at[c, x, pl.ds(0, plane - 1)], 3)
    sent(rx, 4)
    sent(gcb.at[x, pl.ds(0, pgs_n - 1)], 5)
    sent(rx2, 6)
    sent(gr2, 7)
    sent(ca.at[c, x], 8)
    sent(ca.at[c, pl.ds(0, nx - 1)], 9)
    sent(rr.at[pl.ds(0, plane - 1)], 10)
    sent(gr.at[pl.ds(0, pgs_n - 1)], 11)
    sent(gcb.at[pl.ds(0, nx - 1)], 12)
    sent(ca.at[c, pl.ds(0, nx - 1)], 13)


def mega(dims, vec, mor, siz, bas, lt, mt, rt, pairs, lcoup, partner, dcoup, gpart, gcoup):
    nx, ny, nz = dims
    plane, pgn = ny * nz, ny * nz // 4
    b = lambda *s: pltpu.VMEM(s, BF16)
    vm = pl.BlockSpec(memory_space=pltpu.VMEM)
    scratch = [
        b(512, 4096), VM((32, 1024), F32), b(512, 32), VM((64, 1024), F32), VM((1024, 2), F32), b(1024, 32), b(1024, 32),
        b(2, nx, plane, 4, 128), b(2, nx, plane, 4, 128), b(nx, plane, 4, 128), b(nx, plane, 4, 128),
        b(nx - 1, plane, 4, 128), b(plane, 4, 128), b(plane, 4, 128),
        b(8, 4, 128), b(8, 4, 1024), VM((8, 1, 128), I32),
        b(nx, pgn, 4, 128), b(nx, pgn, 4, 128), b(nx - 1, pgn, 4, 128), b(pgn, 4, 128), b(pgn, 4, 128),
        b(1024, 512), b(4, 128), b(4, 128), VM((1, 128), I32), b(4, 128),
        pltpu.SemaphoreType.DMA((14,)), pltpu.SemaphoreType.DMA((14,)),
    ]
    return pl.pallas_call(
        functools.partial(mega_kernel, dims),
        out_shape=(S((16, 32), BF16), S((512, 32), F32)),
        in_specs=[vm] * 13,
        scratch_shapes=scratch,
        compiler_params=pltpu.CompilerParams(collective_id=0, has_side_effects=True),
    )(vec, mor, siz, bas, lt, mt, rt, pairs, lcoup, partner, dcoup, gpart, gcoup)


def body(dims, vec, mor, siz, bas, lt, mt, rt, pairs, lcoup, partner, dcoup, gpart, gcoup):
    top, far = mega(dims, vec, mor, siz, bas, lt, mt, rt, pairs, lcoup, partner, dcoup, gpart, gcoup)
    return down(top, far, mor, siz, bas, lt, mt)


def solution(mesh):
    split = Mesh(mesh.devices.reshape(4, 8, 8, 2), AXES)
    rows, cols = P(AXES, None), P(None, AXES)
    in_specs = (cols, rows, rows, cols, rows, rows, rows, cols, rows, rows, rows, rows, rows)
    step = functools.partial(body, (4, 8, 8))
    return jax.shard_map(step, mesh=split, in_specs=in_specs, out_specs=cols, check_vma=False)
```

```python
import functools
import jax
import jax.numpy as jnp
from jax import lax
from jax.experimental import pallas as pl
from jax.experimental.pallas import tpu as pltpu
from jax.sharding import Mesh
from jax.sharding import PartitionSpec as P

F32, BF16, I32 = jnp.float32, jnp.bfloat16, jnp.int32
NT = (((1,), (1,)), ((), ()))
TN = (((0,), (0,)), ((), ()))


def iota(shape, dim):
    return lax.broadcasted_iota(I32, shape, dim)


def dot(a, b, dims=(((1,), (0,)), ((), ()))):
    return lax.dot_general(a, b, dims, preferred_element_type=F32)


def hot(mask):
    return jnp.where(mask, 1.0, 0.0).astype(BF16)


def spread_row():
    return hot(iota((32, 1024), 1) // 32 == iota((32, 1024), 0))


def spread_col():
    return hot(iota((32, 1024), 1) % 32 == iota((32, 1024), 0))


def fold_first(x):
    w = x[:, 0:128]
    for q in range(1, 8):
        w = w + x[:, q * 128 : (q + 1) * 128]
    return (w[:, 0:32] + w[:, 32:64]) + (w[:, 64:96] + w[:, 96:128])


def leaf_of(siz_ref, start, width):
    sizes = siz_ref[...].astype(F32)
    lower = iota((32, 32), 1) <= iota((32, 32), 0)
    ends = jnp.sum(jnp.where(lower, jnp.broadcast_to(sizes, (32, 32)), 0.0), axis=1, keepdims=True)
    pos = (iota((32, width), 1) + start).astype(F32)
    return jnp.sum(jnp.where(pos >= ends, 1.0, 0.0), axis=0, keepdims=True)


CH = 1024


def down_kernel(top, far, mor, siz, bas, lt, mt, out):
    erow, ecol = spread_row(), spread_col()
    back = hot(iota((1024, 32), 0) // 32 == iota((1024, 32), 1))
    xt = dot(top[...], ecol)
    p = jnp.concatenate([xt * mt[m : m + 1, :].astype(F32) for m in range(4)], axis=0)
    ph = p.astype(BF16)
    pl_ = (p - ph.astype(F32)).astype(BF16)
    mid = (dot(ph, back) + dot(pl_, back)).astype(BF16)
    tots = []
    for m in range(4):
        x = dot(mid[m * 16 : (m + 1) * 16], ecol)
        q = jnp.concatenate(
            [x * lt[m * 8 + l : m * 8 + l + 1, :].astype(F32) for l in range(8)], axis=0
        ).astype(BF16)
        tots.append((dot(q, back) + far[m * 128 : (m + 1) * 128, :]).astype(BF16))
    tot = jnp.concatenate(tots, axis=0)

    def chunk(c, acc):
        at = pl.multiple_of(c * CH, CH)
        m = mor[:, pl.ds(at, CH)]
        lo, hi = m & 255, m >> 8
        pick = hot(iota((256, CH), 0) == lo)
        wide = dot(tot, bas[:, pl.ds(at, CH)])
        leaf = jnp.broadcast_to(leaf_of(siz, at, CH), (16, CH))
        o = wide[0:16]
        for l in range(1, 32):
            o = jnp.where(leaf == l, wide[l * 16 : (l + 1) * 16], o)
        ob = o.astype(BF16)
        hib = jnp.broadcast_to(hi, (16, CH)).astype(F32).astype(BF16)
        scat = jnp.concatenate([jnp.where(hib == h, ob, jnp.zeros((), BF16)) for h in range(16)], axis=0)
        return acc + dot(scat, pick, NT)

    acc = lax.fori_loop(0, 4096 // CH, chunk, jnp.zeros((256, 256), F32), unroll=2)
    for h in range(16):
        out[:, h * 256 : (h + 1) * 256] = acc[h * 16 : (h + 1) * 16]


S = jax.ShapeDtypeStruct
VM = pltpu.VMEM


def down(top, far, mor, siz, bas, lt, mt):
    return pl.pallas_call(down_kernel, out_shape=S((16, 4096), F32))(top, far, mor, siz, bas, lt, mt)


AXES = ("leaf_0", "leaf_1", "leaf_2", "leaf_3")
MESH = pl.DeviceIdType.MESH


def split2(x):
    hi = x.astype(BF16)
    return hi, (x - hi.astype(F32)).astype(BF16)


def pack_row(c):
    wide = dot(c, hot(iota((32, 128), 1) % 32 == iota((32, 128), 0)))
    wide = jnp.where(iota((16, 128), 1) // 32 == iota((16, 128), 0) % 4, wide, 0.0).astype(BF16)
    return dot(hot(iota((4, 16), 1) // 4 == iota((4, 16), 0)), wide)


def unpack_row(r):
    sel = hot(iota((16, 4), 0) // 4 == iota((16, 4), 1))
    hi, lo = split2(r)
    wide = dot(sel, hi) + dot(sel, lo)
    wide = jnp.where(iota((16, 128), 1) // 32 == iota((16, 128), 0) % 4, wide, 0.0)
    return (wide[:, 0:32] + wide[:, 32:64]) + (wide[:, 64:96] + wide[:, 96:128])


def sum_rows(ref, n):
    flat = ref[...].reshape(n * 4, 128)
    return dot(hot(iota((4, n * 4), 1) % 4 == iota((4, n * 4), 0)), flat)


def back_weights(c, w):
    cex = dot(c, hot(iota((16, 512), 1) // 32 == iota((16, 512), 0)), TN)
    same = iota((32, 512), 1) % 32 == iota((32, 512), 0)
    for i in range(32):
        row = jnp.broadcast_to(cex[i : i + 1, :], (32, 512))
        w[i * 32 : (i + 1) * 32, :] = jnp.where(same, row, 0.0).astype(BF16)


def forward_sum(blocks, chosen):
    same = iota((32, 512), 1) % 32 == iota((32, 512), 0)
    rows = []
    for q in range(4):
        part = dot(blocks[:, q * 256 : (q + 1) * 256], chosen, TN)
        for i in range(8):
            rows.append(jnp.sum(jnp.where(same, part[i * 32 : (i + 1) * 32], 0.0), axis=0, keepdims=True))
    y = jnp.concatenate(rows, axis=0)
    hi, lo = split2(y)
    sel = hot(iota((16, 512), 1) // 32 == iota((16, 512), 0))
    return dot(sel, hi, NT) + dot(sel, lo, NT)


UP = 512


def lanes_of(x):
    return x.reshape(x.shape[0], 512)


def add_all(terms):
    return functools.reduce(lambda a, b: a + b, [t.astype(F32) for t in terms]).astype(BF16)


def mega_kernel(dims, *refs):
    ins, (top_out, far_out), rest = refs[:13], refs[13:15], refs[15:]
    staged, (inputs, *rest) = rest[:13], rest[13:]
    mega_body(dims, ins, staged, inputs, top_out, far_out, *rest)


def mega_body(dims, ins, staged, inputs, top_out, far_out,
                masked, lt32, lc, s32, idcol, fwd, bwd,
                ca, rsb, rx, sb, rx2, sb2, rr, gx, sgx, pgx, gcb, tb, gr2, tb2, gr, w,
                rowb, termb, pgs, gcrow, send, recv):
    loads = [pltpu.make_async_copy(a, b, inputs.at[i]) for i, (a, b) in enumerate(zip(ins, staged))]
    for load in loads:
        load.start()
    vec, mor, siz, bas, lt, mt, rt, pairs, lcoup, partner, dcoup, gpart, gcoup = staged
    nx, ny, nz = dims
    halves = nz // 4
    plane, pgs_n = ny * nz, ny * halves
    x, y, z, c = [lax.axis_index(a) for a in AXES]
    zq, zh = z % 4, z // 4
    k = zq * 2 + c
    yz = y * nz + z
    pg = y * halves + zh
    xs = [(x + j) % nx for j in range(nx)]
    ys = [(y + j) % ny for j in range(ny)]
    zs = [(z + j) % nz for j in range(nz)]
    gz = [((zh + j) % halves) * 4 + zq for j in range(halves)]
    far_first = lambda o: -(min(o[0], ny - o[0]) + min(o[1], nz - o[1]))
    offs = sorted([(a, b) for a in range(ny) for b in range(nz) if a or b], key=far_first)
    goffs = sorted([(a, b) for a in range(ny) for b in range(halves) if a or b], key=lambda o: -min(o[0], ny - o[0]))
    sibling = (x, y, z, 1 - c)

    def mate(j):
        r = (k + j) % 8
        return (x, y, zh * 4 + r // 2, r % 2)

    def push(src, dst, i, to):
        pltpu.make_async_remote_copy(src, dst, send.at[i], recv.at[i], device_id=to, device_id_type=MESH).start()

    def settle(ref, i, which):
        cp = pltpu.make_async_remote_copy(
            ref, ref, send.at[i], recv.at[i], device_id=sibling, device_id_type=MESH
        )
        (cp.wait_recv if which else cp.wait_send)()

    def got(ref, i):
        settle(ref, i, True)

    def sent(ref, i):
        settle(ref, i, False)

    bar = pltpu.get_barrier_semaphore()

    def greet(to):
        pl.semaphore_signal(bar, inc=1, device_id=to, device_id_type=MESH)

    for a, b in offs:
        greet((x, ys[a], zs[b], c))
    for j in range(1, nx):
        greet((xs[j], y, z, c))
    for j in range(1, 8):

        @pl.when((k + j) % 2 != c)
        def _():
            greet(mate(j))

    for i in (0, 1, 2):
        loads[i].wait()
    vx = jnp.concatenate([vec[:, h * 256 : (h + 1) * 256] for h in range(16)], axis=0).astype(BF16)

    def chunk(i, carry):
        at = pl.multiple_of(i * UP, UP)
        m = mor[:, pl.ds(at, UP)]
        lo, hi = m & 255, m >> 8
        wide = dot(vx, hot(iota((256, UP), 0) == lo))
        hib = jnp.broadcast_to(hi, (16, UP))
        sv = wide[0:16]
        for h in range(1, 16):
            sv = jnp.where(hib == h, wide[h * 16 : (h + 1) * 16], sv)
        leaf = jnp.broadcast_to(leaf_of(siz, at, UP), (16, UP)).astype(BF16)
        svb = sv.astype(BF16)
        for l in range(32):
            masked[l * 16 : (l + 1) * 16, pl.ds(at, UP)] = jnp.where(leaf == l, svb, jnp.zeros((), BF16))
        return carry

    lax.fori_loop(0, 4096 // UP, chunk, 0, unroll=2)
    for load in loads[3:]:
        load.wait()
    pgs[...] = jnp.zeros((1, 128), I32)
    pgs[:, 0:4] = gpart[...]
    lt32[...] = lt[...].astype(F32)
    lcv = dot(bas[...], masked[...], NT).astype(BF16)
    lc[...] = lcv
    erow, ecol = spread_row(), spread_col()
    root = jnp.zeros((16, 1024), F32)
    for m in range(4):
        acc = jnp.zeros((16, 1024), F32)
        wide = dot(lcv[:, m * 128 : (m + 1) * 128], erow, TN)
        for l in range(8):
            acc = acc + wide[l * 16 : (l + 1) * 16] * lt32[m * 8 + l : m * 8 + l + 1, :]
        mid = fold_first(acc).astype(BF16)
        root = root + dot(mid, erow) * mt[m : m + 1, :].astype(F32)
    root = fold_first(root).astype(BF16)
    term = fold_first(dot(root, erow) * rt[...].astype(F32)).astype(BF16)
    termb[...] = pack_row(term).astype(BF16)
    rowb[...] = pack_row(root).astype(BF16)
    pl.semaphore_wait(bar, plane - 1 + nx - 1 + 4)

    for j in range(1, 8):
        push(termb, gx.at[k], 0, mate(j))
    for a, b in offs:
        push(rowb, ca.at[c, x, yz], 3, (x, ys[a], zs[b], c))
    for j in range(1, 8):
        push(gcoup, sgx.at[k], 1, mate(j))
        push(pgs, pgx.at[k], 2, mate(j))
    gx[k] = termb[...]
    sgx[k] = gcoup[...]
    pgx[k] = pgs[...]
    ca[c, x, yz] = rowb[...]

    back_weights(root, w)
    bk = dot(dcoup[...], w[...]).astype(BF16)
    chips = nx * plane
    for half in range(2):
        ids = iota((chips, 128), 0) * 2 + half
        hotb = hot(ids == jnp.broadcast_to(partner[...], (chips, 128)))
        rsb[half] = dot(hotb, bk).astype(BF16).reshape(nx, plane, 4, 128)
    push(rsb.at[1 - c], rx, 4, sibling)

    got(rx, 4)
    sb[...] = add_all([rsb[c], rx[...]])
    for j in range(1, nx):
        push(sb.at[xs[j]], rx2.at[j - 1], 6, (xs[j], y, z, c))

    got(gx.at[pl.ds(0, 7)], 0)
    gcoef = sum_rows(gx, 8).astype(BF16)
    gcrow[...] = gcoef
    for a, b in goffs:
        push(gcrow, gcb.at[x, pg], 5, (x, ys[a], gz[b], c))
    gcb[x, pg] = gcoef

    got(sgx.at[pl.ds(0, 7)], 1)
    got(pgx.at[pl.ds(0, 7)], 2)
    sg = sgx[...].reshape(32, 1024)
    groups = nx * pgs_n
    p8 = pgx[...].reshape(8, 128).astype(F32).astype(BF16)[:, 0:4]
    spread = dot(p8, hot(iota((4, 32), 1) % 4 == iota((4, 32), 0)))
    gpair = jnp.sum(jnp.where(iota((8, 32), 1) // 4 == iota((8, 32), 0), spread, 0.0), axis=0, keepdims=True)
    hotg = hot(iota((groups, 32), 0).astype(F32) == jnp.broadcast_to(gpair, (groups, 32)))
    back_weights(unpack_row(gcoef.astype(F32)).astype(BF16), w)
    tb[...] = dot(hotg, dot(sg, w[...]).astype(BF16)).astype(BF16).reshape(nx, pgs_n, 4, 128)
    for j in range(1, nx):
        push(tb.at[xs[j]], gr2.at[j - 1], 7, (xs[j], y, z, c))

    s32[...] = lcoup[...].astype(F32)
    each = hot(iota((64, 1024), 1) // 16 == iota((64, 1024), 0))
    pairsb = pairs[...].astype(F32).astype(BF16)
    idcol[...] = dot(each, pairsb, (((0,), (1,)), ((), ())))
    back = hot(iota((1024, 32), 0) // 32 == iota((1024, 32), 1))

    def leaf_group(gi, carry):
        at = pl.multiple_of(gi * 256, 256)
        eye = iota((256, 512), 0) % 16 == iota((256, 512), 1) % 16
        for which, e in ((1, ecol), (0, erow)):
            leaf = jnp.broadcast_to(idcol[pl.ds(at, 256), which : which + 1], (256, 512))
            here = hot(eye & (leaf == (iota((256, 512), 1) // 16).astype(F32)))
            wide = dot(dot(here, lc[...], NT).astype(BF16), e)
            parts = [wide[t * 16 : (t + 1) * 16] * s32[pl.ds(gi * 16 + t, 1), :] for t in range(16)]
            if which == 1:
                out = dot(jnp.concatenate(parts, axis=0).astype(BF16), back)
                fwd[pl.ds(at, 256), :] = out.astype(BF16)
            else:
                out = jnp.concatenate([fold_first(t) for t in parts], axis=0)
                bwd[pl.ds(at, 256), :] = out.astype(BF16)
        return carry

    lax.fori_loop(0, 2, leaf_group, 0)

    got(ca.at[c, x, pl.ds(0, plane - 1)], 3)
    for j in range(1, nx):
        push(ca.at[c, x], ca.at[c, x], 13 + j, (xs[j], y, z, c))
    push(ca.at[c, x], ca.at[c, x], 8, sibling)

    got(rx2, 6)
    sb2[...] = add_all([sb[x]] + [rx2[j] for j in range(nx - 1)])
    for a, b in offs:
        push(sb2.at[ys[a] * nz + zs[b]], rr.at[yz], 10, (x, ys[a], zs[b], c))
    rr[yz] = sb2[yz]
    got(gr2, 7)
    tb2[...] = add_all([tb[x]] + [gr2[j] for j in range(nx - 1)])
    for a, b in goffs:
        push(tb2.at[ys[a] * halves + (zh + b) % halves], gr.at[pg], 11, (x, ys[a], gz[b], c))
    gr[pg] = tb2[pg]

    got(gcb.at[x, pl.ds(0, pgs_n - 1)], 5)
    for j in range(1, nx):
        push(gcb.at[x], gcb.at[x], 12, (xs[j], y, z, c))

    lax.fori_loop(2, 4, leaf_group, 0)

    ids = dot(pairsb, each)
    same = iota((512, 1024), 0) % 16 == iota((512, 1024), 1) % 16
    leaf = (iota((512, 1024), 0) // 16).astype(F32)
    far_out[...] = dot(hot(same & (leaf == ids[0:1])), fwd[...]) + dot(hot(same & (leaf == ids[1:2])), bwd[...])

    for j in sorted(range(1, nx), key=lambda j: min(j, nx - j)):
        got(ca.at[c, x], 13 + j)
        push(ca.at[c, xs[-j]], ca.at[c, xs[-j]], 13, sibling)
    got(gcb.at[pl.ds(0, nx - 1)], 12)
    far = dot(hotg, lanes_of(gcb[...].reshape(groups, 4, 128)), TN).astype(BF16)
    group_far = forward_sum(sg, far)
    got(ca.at[c, x], 8)
    got(ca.at[c, pl.ds(0, nx - 1)], 13)
    near = jnp.zeros((128, 512), F32)
    for half in range(2):
        ids = iota((chips, 128), 0) * 2 + half
        hotb = hot(ids == jnp.broadcast_to(partner[...], (chips, 128)))
        near = near + dot(hotb, lanes_of(ca[half].reshape(chips, 4, 128)), TN)
    root_far = forward_sum(dcoup[...], near.astype(BF16))

    got(rr.at[pl.ds(0, plane - 1)], 10)
    root_far = root_far + unpack_row(sum_rows(rr, plane))
    got(gr.at[pl.ds(0, pgs_n - 1)], 11)
    group_far = (group_far + unpack_row(sum_rows(gr, pgs_n))).astype(BF16)
    hi, lo = split2(dot(group_far, ecol) * rt[...].astype(F32))
    top_out[...] = (root_far + dot(hi, back) + dot(lo, back)).astype(BF16)

    sent(gx.at[pl.ds(0, 7)], 0)
    sent(sgx.at[pl.ds(0, 7)], 1)
    sent(pgx.at[pl.ds(0, 7)], 2)
    sent(ca.at[c, x, pl.ds(0, plane - 1)], 3)
    sent(rx, 4)
    sent(gcb.at[x, pl.ds(0, pgs_n - 1)], 5)
    sent(rx2, 6)
    sent(gr2, 7)
    sent(ca.at[c, x], 8)
    for j in range(1, nx):
        sent(ca.at[c, x], 13 + j)
    sent(rr.at[pl.ds(0, plane - 1)], 10)
    sent(gr.at[pl.ds(0, pgs_n - 1)], 11)
    sent(gcb.at[pl.ds(0, nx - 1)], 12)
    sent(ca.at[c, pl.ds(0, nx - 1)], 13)


def mega(dims, vec, mor, siz, bas, lt, mt, rt, pairs, lcoup, partner, dcoup, gpart, gcoup):
    nx, ny, nz = dims
    plane, pgn = ny * nz, ny * nz // 4
    b = lambda *s: pltpu.VMEM(s, BF16)
    ins = (vec, mor, siz, bas, lt, mt, rt, pairs, lcoup, partner, dcoup, gpart, gcoup)
    scratch = [
        b(512, 4096), VM((32, 1024), F32), b(32, 512), VM((64, 1024), F32), VM((1024, 2), F32), b(1024, 32), b(1024, 32),
        b(2, nx, plane, 4, 128), b(2, nx, plane, 4, 128), b(nx, plane, 4, 128), b(nx, plane, 4, 128),
        b(nx - 1, plane, 4, 128), b(plane, 4, 128), b(plane, 4, 128),
        b(8, 4, 128), b(8, 4, 1024), VM((8, 1, 128), I32),
        b(nx, pgn, 4, 128), b(nx, pgn, 4, 128), b(nx - 1, pgn, 4, 128), b(pgn, 4, 128), b(pgn, 4, 128),
        b(1024, 512), b(4, 128), b(4, 128), VM((1, 128), I32), b(4, 128),
        pltpu.SemaphoreType.DMA((13 + nx,)), pltpu.SemaphoreType.DMA((13 + nx,)),
    ]
    return pl.pallas_call(
        functools.partial(mega_kernel, dims),
        out_shape=(S((16, 32), BF16), S((512, 32), F32)),
        in_specs=[pl.BlockSpec(memory_space=pl.ANY)] * 13,
        scratch_shapes=[VM(a.shape, a.dtype) for a in ins] + [pltpu.SemaphoreType.DMA((13,))] + scratch,
        compiler_params=pltpu.CompilerParams(collective_id=0, has_side_effects=True),
    )(*ins)


def body(dims, vec, mor, siz, bas, lt, mt, rt, pairs, lcoup, partner, dcoup, gpart, gcoup):
    top, far = mega(dims, vec, mor, siz, bas, lt, mt, rt, pairs, lcoup, partner, dcoup, gpart, gcoup)
    return down(top, far, mor, siz, bas, lt, mt)


def solution(mesh):
    split = Mesh(mesh.devices.reshape(4, 8, 8, 2), AXES)
    rows, cols = P(AXES, None), P(None, AXES)
    in_specs = (cols, rows, rows, cols, rows, rows, rows, cols, rows, rows, rows, rows, rows)
    step = functools.partial(body, (4, 8, 8))
    return jax.shard_map(step, mesh=split, in_specs=in_specs, out_specs=cols, check_vma=False)
```

```python
import functools
import jax
import jax.numpy as jnp
from jax import lax
from jax.experimental import pallas as pl
from jax.experimental.pallas import tpu as pltpu
from jax.sharding import Mesh
from jax.sharding import PartitionSpec as P

F32, BF16, I32 = jnp.float32, jnp.bfloat16, jnp.int32
NT = (((1,), (1,)), ((), ()))
TN = (((0,), (0,)), ((), ()))


def iota(shape, dim):
    return lax.broadcasted_iota(I32, shape, dim)


def dot(a, b, dims=(((1,), (0,)), ((), ()))):
    return lax.dot_general(a, b, dims, preferred_element_type=F32)


def hot(mask):
    return jnp.where(mask, 1.0, 0.0).astype(BF16)


def spread_row():
    return hot(iota((32, 1024), 1) // 32 == iota((32, 1024), 0))


def spread_col():
    return hot(iota((32, 1024), 1) % 32 == iota((32, 1024), 0))


def fold_first(x):
    w = x[:, 0:128]
    for q in range(1, 8):
        w = w + x[:, q * 128 : (q + 1) * 128]
    return (w[:, 0:32] + w[:, 32:64]) + (w[:, 64:96] + w[:, 96:128])


def leaf_of(siz_ref, start, width):
    sizes = siz_ref[...].astype(F32)
    lower = iota((32, 32), 1) <= iota((32, 32), 0)
    ends = jnp.sum(jnp.where(lower, jnp.broadcast_to(sizes, (32, 32)), 0.0), axis=1, keepdims=True)
    pos = (iota((32, width), 1) + start).astype(F32)
    return jnp.sum(jnp.where(pos >= ends, 1.0, 0.0), axis=0, keepdims=True)


CH = 1024


def down_kernel(top, far, mor, siz, bas, lt, mt, out):
    erow, ecol = spread_row(), spread_col()
    back = hot(iota((1024, 32), 0) // 32 == iota((1024, 32), 1))
    xt = dot(top[...], ecol)
    p = jnp.concatenate([xt * mt[m : m + 1, :].astype(F32) for m in range(4)], axis=0)
    ph = p.astype(BF16)
    pl_ = (p - ph.astype(F32)).astype(BF16)
    mid = (dot(ph, back) + dot(pl_, back)).astype(BF16)
    tots = []
    for m in range(4):
        x = dot(mid[m * 16 : (m + 1) * 16], ecol)
        q = jnp.concatenate(
            [x * lt[m * 8 + l : m * 8 + l + 1, :].astype(F32) for l in range(8)], axis=0
        ).astype(BF16)
        tots.append((dot(q, back) + far[m * 128 : (m + 1) * 128, :]).astype(BF16))
    tot = jnp.concatenate(tots, axis=0)

    def chunk(c, acc):
        at = pl.multiple_of(c * CH, CH)
        m = mor[:, pl.ds(at, CH)]
        lo, hi = m & 255, m >> 8
        pick = hot(iota((256, CH), 0) == lo)
        wide = dot(tot, bas[:, pl.ds(at, CH)])
        leaf = jnp.broadcast_to(leaf_of(siz, at, CH), (16, CH))
        o = wide[0:16]
        for l in range(1, 32):
            o = jnp.where(leaf == l, wide[l * 16 : (l + 1) * 16], o)
        ob = o.astype(BF16)
        hib = jnp.broadcast_to(hi, (16, CH)).astype(F32).astype(BF16)
        scat = jnp.concatenate([jnp.where(hib == h, ob, jnp.zeros((), BF16)) for h in range(16)], axis=0)
        return acc + dot(scat, pick, NT)

    acc = lax.fori_loop(0, 4096 // CH, chunk, jnp.zeros((256, 256), F32), unroll=2)
    for h in range(16):
        out[:, h * 256 : (h + 1) * 256] = acc[h * 16 : (h + 1) * 16]


S = jax.ShapeDtypeStruct
VM = pltpu.VMEM


def down(top, far, mor, siz, bas, lt, mt):
    return pl.pallas_call(down_kernel, out_shape=S((16, 4096), F32))(top, far, mor, siz, bas, lt, mt)


AXES = ("leaf_0", "leaf_1", "leaf_2", "leaf_3")
MESH = pl.DeviceIdType.MESH


def split2(x):
    hi = x.astype(BF16)
    return hi, (x - hi.astype(F32)).astype(BF16)


def pack_row(c):
    wide = dot(c, hot(iota((32, 128), 1) % 32 == iota((32, 128), 0)))
    wide = jnp.where(iota((16, 128), 1) // 32 == iota((16, 128), 0) % 4, wide, 0.0).astype(BF16)
    return dot(hot(iota((4, 16), 1) // 4 == iota((4, 16), 0)), wide)


def unpack_row(r):
    sel = hot(iota((16, 4), 0) // 4 == iota((16, 4), 1))
    hi, lo = split2(r)
    wide = dot(sel, hi) + dot(sel, lo)
    wide = jnp.where(iota((16, 128), 1) // 32 == iota((16, 128), 0) % 4, wide, 0.0)
    return (wide[:, 0:32] + wide[:, 32:64]) + (wide[:, 64:96] + wide[:, 96:128])


def sum_rows(ref, n):
    flat = ref[...].reshape(n * 4, 128)
    return dot(hot(iota((4, n * 4), 1) % 4 == iota((4, n * 4), 0)), flat)


def back_weights(c, w):
    cex = dot(c, hot(iota((16, 512), 1) // 32 == iota((16, 512), 0)), TN)
    same = iota((32, 512), 1) % 32 == iota((32, 512), 0)
    for i in range(32):
        row = jnp.broadcast_to(cex[i : i + 1, :], (32, 512))
        w[i * 32 : (i + 1) * 32, :] = jnp.where(same, row, 0.0).astype(BF16)


def forward_sum(blocks, chosen):
    same = iota((32, 512), 1) % 32 == iota((32, 512), 0)
    rows = []
    for q in range(4):
        part = dot(blocks[:, q * 256 : (q + 1) * 256], chosen, TN)
        for i in range(8):
            rows.append(jnp.sum(jnp.where(same, part[i * 32 : (i + 1) * 32], 0.0), axis=0, keepdims=True))
    y = jnp.concatenate(rows, axis=0)
    hi, lo = split2(y)
    sel = hot(iota((16, 512), 1) // 32 == iota((16, 512), 0))
    return dot(sel, hi, NT) + dot(sel, lo, NT)


UP = 512


def lanes_of(x):
    return x.reshape(x.shape[0], 512)


def add_all(terms):
    return functools.reduce(lambda a, b: a + b, [t.astype(F32) for t in terms]).astype(BF16)


def mega_kernel(dims, *refs):
    ins, (top_out, far_out), rest = refs[:13], refs[13:15], refs[15:]
    staged, (inputs, *rest) = rest[:13], rest[13:]
    mega_body(dims, ins, staged, inputs, top_out, far_out, *rest)


def mega_body(dims, ins, staged, inputs, top_out, far_out,
                masked, lt32, lc, s32, idcol, leaf_far,
                ca, rsb, rx, sb, rx2, sb2, rr, gx, sgx, pgx, gcb, tb, gr2, tb2, gr, w,
                rowb, termb, pgs, gcrow, send, recv):
    loads = [pltpu.make_async_copy(a, b, inputs.at[i]) for i, (a, b) in enumerate(zip(ins, staged))]
    for load in loads:
        load.start()
    vec, mor, siz, bas, lt, mt, rt, pairs, lcoup, partner, dcoup, gpart, gcoup = staged
    nx, ny, nz = dims
    halves = nz // 4
    plane, pgs_n = ny * nz, ny * halves
    x, y, z, c = [lax.axis_index(a) for a in AXES]
    zq, zh = z % 4, z // 4
    k = zq * 2 + c
    yz = y * nz + z
    pg = y * halves + zh
    xs = [(x + j) % nx for j in range(nx)]
    ys = [(y + j) % ny for j in range(ny)]
    zs = [(z + j) % nz for j in range(nz)]
    gz = [((zh + j) % halves) * 4 + zq for j in range(halves)]
    far_first = lambda o: -(min(o[0], ny - o[0]) + min(o[1], nz - o[1]))
    offs = sorted([(a, b) for a in range(ny) for b in range(nz) if a or b], key=far_first)
    goffs = sorted([(a, b) for a in range(ny) for b in range(halves) if a or b], key=lambda o: -min(o[0], ny - o[0]))
    near_y = [a for a in range(ny) if min(a, ny - a) <= ny // 4]
    far_y = [a for a in range(ny) if a not in near_y]
    row_of = lambda a: pl.ds(ys[a] * nz, nz)
    sibling = (x, y, z, 1 - c)

    def mate(j):
        r = (k + j) % 8
        return (x, y, zh * 4 + r // 2, r % 2)

    def push(src, dst, i, to):
        pltpu.make_async_remote_copy(src, dst, send.at[i], recv.at[i], device_id=to, device_id_type=MESH).start()

    def settle(ref, i, which):
        cp = pltpu.make_async_remote_copy(
            ref, ref, send.at[i], recv.at[i], device_id=sibling, device_id_type=MESH
        )
        (cp.wait_recv if which else cp.wait_send)()

    def got(ref, i):
        settle(ref, i, True)

    def sent(ref, i):
        settle(ref, i, False)

    bar = pltpu.get_barrier_semaphore()

    def greet(to):
        pl.semaphore_signal(bar, inc=1, device_id=to, device_id_type=MESH)

    for a, b in offs:
        greet((x, ys[a], zs[b], c))
    for j in range(1, nx):
        greet((xs[j], y, z, c))
    for j in range(1, 8):

        @pl.when((k + j) % 2 != c)
        def _():
            greet(mate(j))

    for i in (0, 1, 2):
        loads[i].wait()
    vx = jnp.concatenate([vec[:, h * 256 : (h + 1) * 256] for h in range(16)], axis=0).astype(BF16)

    def chunk(i, carry):
        at = pl.multiple_of(i * UP, UP)
        m = mor[:, pl.ds(at, UP)]
        lo, hi = m & 255, m >> 8
        wide = dot(vx, hot(iota((256, UP), 0) == lo))
        hib = jnp.broadcast_to(hi, (16, UP))
        sv = wide[0:16]
        for h in range(1, 16):
            sv = jnp.where(hib == h, wide[h * 16 : (h + 1) * 16], sv)
        leaf = jnp.broadcast_to(leaf_of(siz, at, UP), (16, UP)).astype(BF16)
        svb = sv.astype(BF16)
        for l in range(32):
            masked[l * 16 : (l + 1) * 16, pl.ds(at, UP)] = jnp.where(leaf == l, svb, jnp.zeros((), BF16))
        return carry

    lax.fori_loop(0, 4096 // UP, chunk, 0, unroll=2)
    for load in loads[3:]:
        load.wait()
    pgs[...] = jnp.zeros((1, 128), I32)
    pgs[:, 0:4] = gpart[...]
    lt32[...] = lt[...].astype(F32)
    lcv = dot(bas[...], masked[...], NT).astype(BF16)
    lc[...] = lcv
    erow, ecol = spread_row(), spread_col()
    root = jnp.zeros((16, 1024), F32)
    for m in range(4):
        acc = jnp.zeros((16, 1024), F32)
        wide = dot(lcv[:, m * 128 : (m + 1) * 128], erow, TN)
        for l in range(8):
            acc = acc + wide[l * 16 : (l + 1) * 16] * lt32[m * 8 + l : m * 8 + l + 1, :]
        mid = fold_first(acc).astype(BF16)
        root = root + dot(mid, erow) * mt[m : m + 1, :].astype(F32)
    root = fold_first(root).astype(BF16)
    rowb[...] = pack_row(root).astype(BF16)
    pl.semaphore_wait(bar, plane - 1 + nx - 1 + 4)

    for a, b in offs:
        push(rowb, ca.at[c, x, yz], 3 if a in near_y else 9, (x, ys[a], zs[b], c))
    term = fold_first(dot(root, erow) * rt[...].astype(F32)).astype(BF16)
    termb[...] = pack_row(term).astype(BF16)
    for j in range(1, 8):
        push(termb, gx.at[k], 0, mate(j))
    for j in range(1, 8):
        push(gcoup, sgx.at[k], 1, mate(j))
        push(pgs, pgx.at[k], 2, mate(j))
    gx[k] = termb[...]
    sgx[k] = gcoup[...]
    pgx[k] = pgs[...]
    ca[c, x, yz] = rowb[...]

    back_weights(root, w)
    bk = dot(dcoup[...], w[...]).astype(BF16)
    chips = nx * plane
    for half in range(2):
        ids = iota((chips, 128), 0) * 2 + half
        hotb = hot(ids == jnp.broadcast_to(partner[...], (chips, 128)))
        rsb[half] = dot(hotb, bk).astype(BF16).reshape(nx, plane, 4, 128)
    push(rsb.at[1 - c], rx, 4, sibling)

    s32[...] = lcoup[...].astype(F32)
    back = hot(iota((1024, 32), 0) // 32 == iota((1024, 32), 1))
    each = hot(iota((64, 1024), 1) // 16 == iota((64, 1024), 0))
    idcol[...] = dot(each, pairs[...].astype(F32).astype(BF16), (((0,), (1,)), ((), ())))

    def leaf_group(gi):
        eye = iota((512, 512), 0) % 16 == iota((512, 512), 1) % 16
        lid = (iota((512, 512), 1) // 16).astype(F32)
        at = slice(gi * 512, gi * 512 + 512)
        first, second = [
            hot(eye & (jnp.broadcast_to(idcol[at, i : i + 1], (512, 512)) == lid)) for i in (0, 1)
        ]
        rows = [s32[gi * 32 + t : gi * 32 + t + 1, :] for t in range(32)]
        wide = dot(dot(second, lc[...], NT).astype(BF16), ecol)
        parts = [wide[t * 16 : (t + 1) * 16] * rows[t] for t in range(32)]
        forth = dot(jnp.concatenate(parts, axis=0).astype(BF16), back).astype(BF16)
        wide = dot(dot(first, lc[...], NT).astype(BF16), erow)
        parts = [fold_first(wide[t * 16 : (t + 1) * 16] * rows[t]) for t in range(32)]
        return dot(forth, first, TN) + dot(jnp.concatenate(parts, axis=0).astype(BF16), second, TN)

    leaf_far[...] = leaf_group(0)

    got(rx, 4)
    sb[...] = add_all([rsb[c], rx[...]])
    for part, i in ((far_y, 6), (near_y, 13 + nx)):
        for a in part:
            for j in range(1, nx):
                push(sb.at[xs[j], row_of(a)], rx2.at[j - 1, row_of(a)], i, (xs[j], y, z, c))

    got(gx.at[pl.ds(0, 7)], 0)
    gcoef = sum_rows(gx, 8).astype(BF16)
    gcrow[...] = gcoef
    for a, b in goffs:
        push(gcrow, gcb.at[x, pg], 5, (x, ys[a], gz[b], c))
    gcb[x, pg] = gcoef

    got(sgx.at[pl.ds(0, 7)], 1)
    got(pgx.at[pl.ds(0, 7)], 2)
    sg = sgx[...].reshape(32, 1024)
    groups = nx * pgs_n
    p8 = pgx[...].reshape(8, 128).astype(F32).astype(BF16)[:, 0:4]
    spread = dot(p8, hot(iota((4, 32), 1) % 4 == iota((4, 32), 0)))
    gpair = jnp.sum(jnp.where(iota((8, 32), 1) // 4 == iota((8, 32), 0), spread, 0.0), axis=0, keepdims=True)
    hotg = hot(iota((groups, 32), 0).astype(F32) == jnp.broadcast_to(gpair, (groups, 32)))
    back_weights(unpack_row(gcoef.astype(F32)).astype(BF16), w)
    tb[...] = dot(hotg, dot(sg, w[...]).astype(BF16)).astype(BF16).reshape(nx, pgs_n, 4, 128)
    for j in range(1, nx):
        push(tb.at[xs[j]], gr2.at[j - 1], 7, (xs[j], y, z, c))

    def along_x(part):
        for a in part:
            for j in range(1, nx):
                push(ca.at[c, x, row_of(a)], ca.at[c, x, row_of(a)], 13 + j, (xs[j], y, z, c))

    got(ca.at[c, x, pl.ds(0, len(near_y) * nz - 1)], 3)
    along_x(near_y)
    got(ca.at[c, x, pl.ds(0, len(far_y) * nz)], 9)
    along_x(far_y)
    push(ca.at[c, x], ca.at[c, x], 8, sibling)

    def over_plane(part, i):
        got(rx2.at[:, pl.ds(0, len(part) * nz)], i)
        for a in part:
            sb2[row_of(a)] = add_all([sb[x, row_of(a)]] + [rx2[j, row_of(a)] for j in range(nx - 1)])
        for a, b in offs:
            if a in part:
                push(sb2.at[ys[a] * nz + zs[b]], rr.at[yz], 10, (x, ys[a], zs[b], c))

    over_plane(far_y, 6)
    got(gr2, 7)
    tb2[...] = add_all([tb[x]] + [gr2[j] for j in range(nx - 1)])
    for a, b in goffs:
        push(tb2.at[ys[a] * halves + (zh + b) % halves], gr.at[pg], 11, (x, ys[a], gz[b], c))
    gr[pg] = tb2[pg]
    over_plane(near_y, 13 + nx)
    rr[yz] = sb2[yz]

    leaf_far[...] += leaf_group(1)

    for j in sorted(range(1, nx), key=lambda j: min(j, nx - j)):
        got(ca.at[c, x], 13 + j)
        push(ca.at[c, xs[-j]], ca.at[c, xs[-j]], 13, sibling)
    got(gcb.at[x, pl.ds(0, pgs_n - 1)], 5)
    for j in range(1, nx):
        push(gcb.at[x], gcb.at[x], 12, (xs[j], y, z, c))
    far_out[...] = leaf_far[...].T
    got(ca.at[c, x], 8)
    got(ca.at[c, pl.ds(0, nx - 1)], 13)
    near = jnp.zeros((128, 512), F32)
    for half in range(2):
        ids = iota((chips, 128), 0) * 2 + half
        hotb = hot(ids == jnp.broadcast_to(partner[...], (chips, 128)))
        near = near + dot(hotb, lanes_of(ca[half].reshape(chips, 4, 128)), TN)
    root_far = forward_sum(dcoup[...], near.astype(BF16))
    got(gcb.at[pl.ds(0, nx - 1)], 12)
    far = dot(hotg, lanes_of(gcb[...].reshape(groups, 4, 128)), TN).astype(BF16)
    group_far = forward_sum(sg, far)
    got(gr.at[pl.ds(0, pgs_n - 1)], 11)
    group_far = (group_far + unpack_row(sum_rows(gr, pgs_n))).astype(BF16)
    got(rr.at[pl.ds(0, plane - 1)], 10)
    root_far = root_far + unpack_row(sum_rows(rr, plane))
    hi, lo = split2(dot(group_far, ecol) * rt[...].astype(F32))
    top_out[...] = (root_far + dot(hi, back) + dot(lo, back)).astype(BF16)

    sent(gx.at[pl.ds(0, 7)], 0)
    sent(sgx.at[pl.ds(0, 7)], 1)
    sent(pgx.at[pl.ds(0, 7)], 2)
    sent(ca.at[c, x, pl.ds(0, len(near_y) * nz - 1)], 3)
    sent(ca.at[c, x, pl.ds(0, len(far_y) * nz)], 9)
    sent(rx, 4)
    sent(gcb.at[x, pl.ds(0, pgs_n - 1)], 5)
    sent(rx2.at[:, pl.ds(0, len(far_y) * nz)], 6)
    sent(rx2.at[:, pl.ds(0, len(near_y) * nz)], 13 + nx)
    sent(gr2, 7)
    sent(ca.at[c, x], 8)
    for j in range(1, nx):
        sent(ca.at[c, x], 13 + j)
    sent(rr.at[pl.ds(0, plane - 1)], 10)
    sent(gr.at[pl.ds(0, pgs_n - 1)], 11)
    sent(gcb.at[pl.ds(0, nx - 1)], 12)
    sent(ca.at[c, pl.ds(0, nx - 1)], 13)


def mega(dims, vec, mor, siz, bas, lt, mt, rt, pairs, lcoup, partner, dcoup, gpart, gcoup):
    nx, ny, nz = dims
    plane, pgn = ny * nz, ny * nz // 4
    b = lambda *s: pltpu.VMEM(s, BF16)
    ins = (vec, mor, siz, bas, lt, mt, rt, pairs, lcoup, partner, dcoup, gpart, gcoup)
    scratch = [
        b(512, 4096), VM((32, 1024), F32), b(32, 512), VM((64, 1024), F32), VM((1024, 2), F32), VM((32, 512), F32),
        b(2, nx, plane, 4, 128), b(2, nx, plane, 4, 128), b(nx, plane, 4, 128), b(nx, plane, 4, 128),
        b(nx - 1, plane, 4, 128), b(plane, 4, 128), b(plane, 4, 128),
        b(8, 4, 128), b(8, 4, 1024), VM((8, 1, 128), I32),
        b(nx, pgn, 4, 128), b(nx, pgn, 4, 128), b(nx - 1, pgn, 4, 128), b(pgn, 4, 128), b(pgn, 4, 128),
        b(1024, 512), b(4, 128), b(4, 128), VM((1, 128), I32), b(4, 128),
        pltpu.SemaphoreType.DMA((14 + nx,)), pltpu.SemaphoreType.DMA((14 + nx,)),
    ]
    return pl.pallas_call(
        functools.partial(mega_kernel, dims),
        out_shape=(S((16, 32), BF16), S((512, 32), F32)),
        in_specs=[pl.BlockSpec(memory_space=pl.ANY)] * 13,
        scratch_shapes=[VM(a.shape, a.dtype) for a in ins] + [pltpu.SemaphoreType.DMA((13,))] + scratch,
        compiler_params=pltpu.CompilerParams(collective_id=0, has_side_effects=True),
    )(*ins)


def body(dims, vec, mor, siz, bas, lt, mt, rt, pairs, lcoup, partner, dcoup, gpart, gcoup):
    top, far = mega(dims, vec, mor, siz, bas, lt, mt, rt, pairs, lcoup, partner, dcoup, gpart, gcoup)
    return down(top, far, mor, siz, bas, lt, mt)


def solution(mesh):
    split = Mesh(mesh.devices.reshape(4, 8, 8, 2), AXES)
    rows, cols = P(AXES, None), P(None, AXES)
    in_specs = (cols, rows, rows, cols, rows, rows, rows, cols, rows, rows, rows, rows, rows)
    step = functools.partial(body, (4, 8, 8))
    return jax.shard_map(step, mesh=split, in_specs=in_specs, out_specs=cols, check_vma=False)
```

```python
import functools
import jax
import jax.numpy as jnp
from jax import lax
from jax.experimental import pallas as pl
from jax.experimental.pallas import tpu as pltpu
from jax.sharding import Mesh
from jax.sharding import PartitionSpec as P

F32, BF16, I32 = jnp.float32, jnp.bfloat16, jnp.int32
NT = (((1,), (1,)), ((), ()))
TN = (((0,), (0,)), ((), ()))


def iota(shape, dim):
    return lax.broadcasted_iota(I32, shape, dim)


def dot(a, b, dims=(((1,), (0,)), ((), ()))):
    return lax.dot_general(a, b, dims, preferred_element_type=F32)


def hot(mask):
    return jnp.where(mask, 1.0, 0.0).astype(BF16)


def spread_row():
    return hot(iota((32, 1024), 1) // 32 == iota((32, 1024), 0))


def spread_col():
    return hot(iota((32, 1024), 1) % 32 == iota((32, 1024), 0))


def fold_first(x):
    w = x[:, 0:128]
    for q in range(1, 8):
        w = w + x[:, q * 128 : (q + 1) * 128]
    return (w[:, 0:32] + w[:, 32:64]) + (w[:, 64:96] + w[:, 96:128])


def leaf_of(siz_ref, start, width):
    sizes = siz_ref[...].astype(F32)
    lower = iota((32, 32), 1) <= iota((32, 32), 0)
    ends = jnp.sum(jnp.where(lower, jnp.broadcast_to(sizes, (32, 32)), 0.0), axis=1, keepdims=True)
    pos = (iota((32, width), 1) + start).astype(F32)
    return jnp.sum(jnp.where(pos >= ends, 1.0, 0.0), axis=0, keepdims=True)


CH = 1024


def down_kernel(top, far, mor, siz, bas, lt, mt, out):
    erow, ecol = spread_row(), spread_col()
    back = hot(iota((1024, 32), 0) // 32 == iota((1024, 32), 1))
    xt = dot(top[...], ecol)
    p = jnp.concatenate([xt * mt[m : m + 1, :].astype(F32) for m in range(4)], axis=0)
    ph = p.astype(BF16)
    pl_ = (p - ph.astype(F32)).astype(BF16)
    mid = (dot(ph, back) + dot(pl_, back)).astype(BF16)
    tots = []
    for m in range(4):
        x = dot(mid[m * 16 : (m + 1) * 16], ecol)
        q = jnp.concatenate(
            [x * lt[m * 8 + l : m * 8 + l + 1, :].astype(F32) for l in range(8)], axis=0
        ).astype(BF16)
        tots.append((dot(q, back) + far[m * 128 : (m + 1) * 128, :]).astype(BF16))
    tot = jnp.concatenate(tots, axis=0)

    def chunk(c, acc):
        at = pl.multiple_of(c * CH, CH)
        m = mor[:, pl.ds(at, CH)]
        lo, hi = m & 255, m >> 8
        pick = hot(iota((256, CH), 0) == lo)
        wide = dot(tot, bas[:, pl.ds(at, CH)])
        leaf = jnp.broadcast_to(leaf_of(siz, at, CH), (16, CH))
        o = wide[0:16]
        for l in range(1, 32):
            o = jnp.where(leaf == l, wide[l * 16 : (l + 1) * 16], o)
        ob = o.astype(BF16)
        hib = jnp.broadcast_to(hi, (16, CH)).astype(F32).astype(BF16)
        scat = jnp.concatenate([jnp.where(hib == h, ob, jnp.zeros((), BF16)) for h in range(16)], axis=0)
        return acc + dot(scat, pick, NT)

    acc = lax.fori_loop(0, 4096 // CH, chunk, jnp.zeros((256, 256), F32), unroll=2)
    for h in range(16):
        out[:, h * 256 : (h + 1) * 256] = acc[h * 16 : (h + 1) * 16]


S = jax.ShapeDtypeStruct
VM = pltpu.VMEM


def down(top, far, mor, siz, bas, lt, mt):
    return pl.pallas_call(down_kernel, out_shape=S((16, 4096), F32))(top, far, mor, siz, bas, lt, mt)


AXES = ("leaf_0", "leaf_1", "leaf_2", "leaf_3")
MESH = pl.DeviceIdType.MESH


def split2(x):
    hi = x.astype(BF16)
    return hi, (x - hi.astype(F32)).astype(BF16)


def pack_row(c):
    wide = dot(c, hot(iota((32, 128), 1) % 32 == iota((32, 128), 0)))
    wide = jnp.where(iota((16, 128), 1) // 32 == iota((16, 128), 0) % 4, wide, 0.0).astype(BF16)
    return dot(hot(iota((4, 16), 1) // 4 == iota((4, 16), 0)), wide)


def unpack_row(r):
    sel = hot(iota((16, 4), 0) // 4 == iota((16, 4), 1))
    hi, lo = split2(r)
    wide = dot(sel, hi) + dot(sel, lo)
    wide = jnp.where(iota((16, 128), 1) // 32 == iota((16, 128), 0) % 4, wide, 0.0)
    return (wide[:, 0:32] + wide[:, 32:64]) + (wide[:, 64:96] + wide[:, 96:128])


def sum_rows(ref, n):
    flat = ref[...].reshape(n * 4, 128)
    return dot(hot(iota((4, n * 4), 1) % 4 == iota((4, n * 4), 0)), flat)


def back_weights(c, w):
    cex = dot(c, hot(iota((16, 512), 1) // 32 == iota((16, 512), 0)), TN)
    same = iota((32, 512), 1) % 32 == iota((32, 512), 0)
    for i in range(32):
        row = jnp.broadcast_to(cex[i : i + 1, :], (32, 512))
        w[i * 32 : (i + 1) * 32, :] = jnp.where(same, row, 0.0).astype(BF16)


def forward_sum(blocks, chosen):
    same = iota((32, 512), 1) % 32 == iota((32, 512), 0)
    rows = []
    for q in range(4):
        part = dot(blocks[:, q * 256 : (q + 1) * 256], chosen, TN)
        for i in range(8):
            rows.append(jnp.sum(jnp.where(same, part[i * 32 : (i + 1) * 32], 0.0), axis=0, keepdims=True))
    y = jnp.concatenate(rows, axis=0)
    hi, lo = split2(y)
    sel = hot(iota((16, 512), 1) // 32 == iota((16, 512), 0))
    return dot(sel, hi, NT) + dot(sel, lo, NT)


UP = 512


def lanes_of(x):
    return x.reshape(x.shape[0], 512)


def add_all(terms):
    return functools.reduce(lambda a, b: a + b, [t.astype(F32) for t in terms]).astype(BF16)


def mega_kernel(dims, *refs):
    ins, (top_out, far_out), rest = refs[:13], refs[13:15], refs[15:]
    staged, (inputs, *rest) = rest[:13], rest[13:]
    mega_body(dims, ins, staged, inputs, top_out, far_out, *rest)


def mega_body(dims, ins, staged, inputs, top_out, far_out,
                masked, lt32, lc, s32, idcol, leaf_far,
                ca, rsb, rx, sb, rx2, sb2, rr, gx, sgx, pgx, gcb, tb, gr2, tb2, gr, w,
                rowb, termb, pgs, gcrow, send, recv):
    loads = [pltpu.make_async_copy(a, b, inputs.at[i]) for i, (a, b) in enumerate(zip(ins, staged))]
    for load in loads:
        load.start()
    vec, mor, siz, bas, lt, mt, rt, pairs, lcoup, partner, dcoup, gpart, gcoup = staged
    nx, ny, nz = dims
    halves = nz // 4
    plane, pgs_n = ny * nz, ny * halves
    x, y, z, c = [lax.axis_index(a) for a in AXES]
    zq, zh = z % 4, z // 4
    k = zq * 2 + c
    yz = y * nz + z
    pg = y * halves + zh
    xs = [(x + j) % nx for j in range(nx)]
    ys = [(y + j) % ny for j in range(ny)]
    zs = [(z + j) % nz for j in range(nz)]
    gz = [((zh + j) % halves) * 4 + zq for j in range(halves)]
    far_first = lambda o: -(min(o[0], ny - o[0]) + min(o[1], nz - o[1]))
    offs = sorted([(a, b) for a in range(ny) for b in range(nz) if a or b], key=far_first)
    goffs = sorted([(a, b) for a in range(ny) for b in range(halves) if a or b], key=lambda o: -min(o[0], ny - o[0]))
    near_y = [a for a in range(ny) if min(a, ny - a) <= ny // 4]
    far_y = [a for a in range(ny) if a not in near_y]
    row_of = lambda a: pl.ds(ys[a] * nz, nz)
    sibling = (x, y, z, 1 - c)

    def mate(j):
        r = (k + j) % 8
        return (x, y, zh * 4 + r // 2, r % 2)

    def push(src, dst, i, to):
        pltpu.make_async_remote_copy(src, dst, send.at[i], recv.at[i], device_id=to, device_id_type=MESH).start()

    def settle(ref, i, which):
        cp = pltpu.make_async_remote_copy(
            ref, ref, send.at[i], recv.at[i], device_id=sibling, device_id_type=MESH
        )
        (cp.wait_recv if which else cp.wait_send)()

    def got(ref, i):
        settle(ref, i, True)

    def sent(ref, i):
        settle(ref, i, False)

    bar = pltpu.get_barrier_semaphore()

    def greet(to):
        pl.semaphore_signal(bar, inc=1, device_id=to, device_id_type=MESH)

    for a, b in offs:
        greet((x, ys[a], zs[b], c))
    for j in range(1, nx):
        greet((xs[j], y, z, c))
    for j in range(1, 8):

        @pl.when((k + j) % 2 != c)
        def _():
            greet(mate(j))

    for i in (0, 1, 2):
        loads[i].wait()
    vx = jnp.concatenate([vec[:, h * 256 : (h + 1) * 256] for h in range(16)], axis=0).astype(BF16)

    def chunk(i, carry):
        at = pl.multiple_of(i * UP, UP)
        m = mor[:, pl.ds(at, UP)]
        lo, hi = m & 255, m >> 8
        wide = dot(vx, hot(iota((256, UP), 0) == lo))
        hib = jnp.broadcast_to(hi, (16, UP))
        sv = wide[0:16]
        for h in range(1, 16):
            sv = jnp.where(hib == h, wide[h * 16 : (h + 1) * 16], sv)
        leaf = jnp.broadcast_to(leaf_of(siz, at, UP), (16, UP)).astype(BF16)
        svb = sv.astype(BF16)
        for l in range(32):
            masked[l * 16 : (l + 1) * 16, pl.ds(at, UP)] = jnp.where(leaf == l, svb, jnp.zeros((), BF16))
        return carry

    lax.fori_loop(0, 4096 // UP, chunk, 0, unroll=2)
    for load in loads[3:]:
        load.wait()
    pgs[...] = jnp.zeros((1, 128), I32)
    pgs[:, 0:4] = gpart[...]
    lt32[...] = lt[...].astype(F32)
    lcv = dot(bas[...], masked[...], NT).astype(BF16)
    lc[...] = lcv
    erow, ecol = spread_row(), spread_col()
    root = jnp.zeros((16, 1024), F32)
    for m in range(4):
        acc = jnp.zeros((16, 1024), F32)
        wide = dot(lcv[:, m * 128 : (m + 1) * 128], erow, TN)
        for l in range(8):
            acc = acc + wide[l * 16 : (l + 1) * 16] * lt32[m * 8 + l : m * 8 + l + 1, :]
        mid = fold_first(acc).astype(BF16)
        root = root + dot(mid, erow) * mt[m : m + 1, :].astype(F32)
    root = fold_first(root).astype(BF16)
    term = fold_first(dot(root, erow) * rt[...].astype(F32)).astype(BF16)
    rowb[...] = pack_row(root).astype(BF16)
    termb[...] = pack_row(term).astype(BF16)
    pl.semaphore_wait(bar, plane - 1 + nx - 1 + 4)

    for j in range(1, 8):
        push(termb, gx.at[k], 0, mate(j))
    for a, b in offs:
        push(rowb, ca.at[c, x, yz], 3 if a in near_y else 9, (x, ys[a], zs[b], c))
    for j in range(1, 8):
        push(gcoup, sgx.at[k], 1, mate(j))
        push(pgs, pgx.at[k], 2, mate(j))
    gx[k] = termb[...]
    sgx[k] = gcoup[...]
    pgx[k] = pgs[...]
    ca[c, x, yz] = rowb[...]

    back_weights(root, w)
    bk = dot(dcoup[...], w[...]).astype(BF16)
    chips = nx * plane
    for half in range(2):
        ids = iota((chips, 128), 0) * 2 + half
        hotb = hot(ids == jnp.broadcast_to(partner[...], (chips, 128)))
        rsb[half] = dot(hotb, bk).astype(BF16).reshape(nx, plane, 4, 128)
    push(rsb.at[1 - c], rx, 4, sibling)

    s32[...] = lcoup[...].astype(F32)
    back = hot(iota((1024, 32), 0) // 32 == iota((1024, 32), 1))
    each = hot(iota((64, 1024), 1) // 16 == iota((64, 1024), 0))
    idcol[...] = dot(each, pairs[...].astype(F32).astype(BF16), (((0,), (1,)), ((), ())))

    def leaf_group(gi):
        eye = iota((512, 512), 0) % 16 == iota((512, 512), 1) % 16
        lid = (iota((512, 512), 1) // 16).astype(F32)
        at = slice(gi * 512, gi * 512 + 512)
        first, second = [
            hot(eye & (jnp.broadcast_to(idcol[at, i : i + 1], (512, 512)) == lid)) for i in (0, 1)
        ]
        rows = [s32[gi * 32 + t : gi * 32 + t + 1, :] for t in range(32)]
        wide = dot(dot(second, lc[...], NT).astype(BF16), ecol)
        parts = [wide[t * 16 : (t + 1) * 16] * rows[t] for t in range(32)]
        forth = dot(jnp.concatenate(parts, axis=0).astype(BF16), back).astype(BF16)
        wide = dot(dot(first, lc[...], NT).astype(BF16), erow)
        parts = [fold_first(wide[t * 16 : (t + 1) * 16] * rows[t]) for t in range(32)]
        return dot(forth, first, TN) + dot(jnp.concatenate(parts, axis=0).astype(BF16), second, TN)

    leaf_far[...] = leaf_group(0)

    got(sgx.at[pl.ds(0, 7)], 1)
    got(pgx.at[pl.ds(0, 7)], 2)
    sg = sgx[...].reshape(32, 1024)
    groups = nx * pgs_n
    p8 = pgx[...].reshape(8, 128).astype(F32).astype(BF16)[:, 0:4]
    spread = dot(p8, hot(iota((4, 32), 1) % 4 == iota((4, 32), 0)))
    gpair = jnp.sum(jnp.where(iota((8, 32), 1) // 4 == iota((8, 32), 0), spread, 0.0), axis=0, keepdims=True)
    hotg = hot(iota((groups, 32), 0).astype(F32) == jnp.broadcast_to(gpair, (groups, 32)))

    got(rx, 4)
    sb[...] = add_all([rsb[c], rx[...]])
    for part, i in ((far_y, 6), (near_y, 13 + nx)):
        for a in part:
            for j in range(1, nx):
                push(sb.at[xs[j], row_of(a)], rx2.at[j - 1, row_of(a)], i, (xs[j], y, z, c))

    got(gx.at[pl.ds(0, 7)], 0)
    gcoef = sum_rows(gx, 8).astype(BF16)
    gcrow[...] = gcoef
    for a, b in goffs:
        push(gcrow, gcb.at[x, pg], 5, (x, ys[a], gz[b], c))
    gcb[x, pg] = gcoef

    back_weights(unpack_row(gcoef.astype(F32)).astype(BF16), w)
    tb[...] = dot(hotg, dot(sg, w[...]).astype(BF16)).astype(BF16).reshape(nx, pgs_n, 4, 128)
    for j in range(1, nx):
        push(tb.at[xs[j]], gr2.at[j - 1], 7, (xs[j], y, z, c))

    def along_x(part):
        for a in part:
            for j in range(1, nx):
                push(ca.at[c, x, row_of(a)], ca.at[c, x, row_of(a)], 13 + j, (xs[j], y, z, c))

    got(ca.at[c, x, pl.ds(0, len(near_y) * nz - 1)], 3)
    along_x(near_y)
    got(ca.at[c, x, pl.ds(0, len(far_y) * nz)], 9)
    along_x(far_y)
    push(ca.at[c, x], ca.at[c, x], 8, sibling)

    def over_plane(part, i):
        got(rx2.at[:, pl.ds(0, len(part) * nz)], i)
        for a in part:
            sb2[row_of(a)] = add_all([sb[x, row_of(a)]] + [rx2[j, row_of(a)] for j in range(nx - 1)])
        for a, b in offs:
            if a in part:
                push(sb2.at[ys[a] * nz + zs[b]], rr.at[yz], 10, (x, ys[a], zs[b], c))

    over_plane(far_y, 6)
    got(gr2, 7)
    tb2[...] = add_all([tb[x]] + [gr2[j] for j in range(nx - 1)])
    for a, b in goffs:
        push(tb2.at[ys[a] * halves + (zh + b) % halves], gr.at[pg], 11, (x, ys[a], gz[b], c))
    gr[pg] = tb2[pg]
    over_plane(near_y, 13 + nx)
    rr[yz] = sb2[yz]

    leaf_far[...] += leaf_group(1)

    for j in sorted(range(1, nx), key=lambda j: min(j, nx - j)):
        got(ca.at[c, x], 13 + j)
        push(ca.at[c, xs[-j]], ca.at[c, xs[-j]], 13, sibling)
    got(gcb.at[x, pl.ds(0, pgs_n - 1)], 5)
    for j in range(1, nx):
        push(gcb.at[x], gcb.at[x], 12, (xs[j], y, z, c))
    far_out[...] = leaf_far[...].T
    got(ca.at[c, x], 8)
    got(ca.at[c, pl.ds(0, nx - 1)], 13)
    near = jnp.zeros((128, 512), F32)
    for half in range(2):
        ids = iota((chips, 128), 0) * 2 + half
        hotb = hot(ids == jnp.broadcast_to(partner[...], (chips, 128)))
        near = near + dot(hotb, lanes_of(ca[half].reshape(chips, 4, 128)), TN)
    root_far = forward_sum(dcoup[...], near.astype(BF16))
    got(gcb.at[pl.ds(0, nx - 1)], 12)
    far = dot(hotg, lanes_of(gcb[...].reshape(groups, 4, 128)), TN).astype(BF16)
    group_far = forward_sum(sg, far)
    got(gr.at[pl.ds(0, pgs_n - 1)], 11)
    group_far = (group_far + unpack_row(sum_rows(gr, pgs_n))).astype(BF16)
    got(rr.at[pl.ds(0, plane - 1)], 10)
    root_far = root_far + unpack_row(sum_rows(rr, plane))
    hi, lo = split2(dot(group_far, ecol) * rt[...].astype(F32))
    top_out[...] = (root_far + dot(hi, back) + dot(lo, back)).astype(BF16)

    sent(gx.at[pl.ds(0, 7)], 0)
    sent(sgx.at[pl.ds(0, 7)], 1)
    sent(pgx.at[pl.ds(0, 7)], 2)
    sent(ca.at[c, x, pl.ds(0, len(near_y) * nz - 1)], 3)
    sent(ca.at[c, x, pl.ds(0, len(far_y) * nz)], 9)
    sent(rx, 4)
    sent(gcb.at[x, pl.ds(0, pgs_n - 1)], 5)
    sent(rx2.at[:, pl.ds(0, len(far_y) * nz)], 6)
    sent(rx2.at[:, pl.ds(0, len(near_y) * nz)], 13 + nx)
    sent(gr2, 7)
    sent(ca.at[c, x], 8)
    for j in range(1, nx):
        sent(ca.at[c, x], 13 + j)
    sent(rr.at[pl.ds(0, plane - 1)], 10)
    sent(gr.at[pl.ds(0, pgs_n - 1)], 11)
    sent(gcb.at[pl.ds(0, nx - 1)], 12)
    sent(ca.at[c, pl.ds(0, nx - 1)], 13)


def mega(dims, vec, mor, siz, bas, lt, mt, rt, pairs, lcoup, partner, dcoup, gpart, gcoup):
    nx, ny, nz = dims
    plane, pgn = ny * nz, ny * nz // 4
    b = lambda *s: pltpu.VMEM(s, BF16)
    ins = (vec, mor, siz, bas, lt, mt, rt, pairs, lcoup, partner, dcoup, gpart, gcoup)
    scratch = [
        b(512, 4096), VM((32, 1024), F32), b(32, 512), VM((64, 1024), F32), VM((1024, 2), F32), VM((32, 512), F32),
        b(2, nx, plane, 4, 128), b(2, nx, plane, 4, 128), b(nx, plane, 4, 128), b(nx, plane, 4, 128),
        b(nx - 1, plane, 4, 128), b(plane, 4, 128), b(plane, 4, 128),
        b(8, 4, 128), b(8, 4, 1024), VM((8, 1, 128), I32),
        b(nx, pgn, 4, 128), b(nx, pgn, 4, 128), b(nx - 1, pgn, 4, 128), b(pgn, 4, 128), b(pgn, 4, 128),
        b(1024, 512), b(4, 128), b(4, 128), VM((1, 128), I32), b(4, 128),
        pltpu.SemaphoreType.DMA((14 + nx,)), pltpu.SemaphoreType.DMA((14 + nx,)),
    ]
    return pl.pallas_call(
        functools.partial(mega_kernel, dims),
        out_shape=(S((16, 32), BF16), S((512, 32), F32)),
        in_specs=[pl.BlockSpec(memory_space=pl.ANY)] * 13,
        scratch_shapes=[VM(a.shape, a.dtype) for a in ins] + [pltpu.SemaphoreType.DMA((13,))] + scratch,
        compiler_params=pltpu.CompilerParams(collective_id=0, has_side_effects=True),
    )(*ins)


def body(dims, vec, mor, siz, bas, lt, mt, rt, pairs, lcoup, partner, dcoup, gpart, gcoup):
    top, far = mega(dims, vec, mor, siz, bas, lt, mt, rt, pairs, lcoup, partner, dcoup, gpart, gcoup)
    return down(top, far, mor, siz, bas, lt, mt)


def solution(mesh):
    split = Mesh(mesh.devices.reshape(4, 8, 8, 2), AXES)
    rows, cols = P(AXES, None), P(None, AXES)
    in_specs = (cols, rows, rows, cols, rows, rows, rows, cols, rows, rows, rows, rows, rows)
    step = functools.partial(body, (4, 8, 8))
    return jax.shard_map(step, mesh=split, in_specs=in_specs, out_specs=cols, check_vma=False)
```

```python
import functools
import jax
import jax.numpy as jnp
from jax import lax
from jax.experimental import pallas as pl
from jax.experimental.pallas import tpu as pltpu
from jax.sharding import Mesh
from jax.sharding import PartitionSpec as P

F32, BF16, I32 = jnp.float32, jnp.bfloat16, jnp.int32
NT = (((1,), (1,)), ((), ()))
TN = (((0,), (0,)), ((), ()))


def iota(shape, dim):
    return lax.broadcasted_iota(I32, shape, dim)


def dot(a, b, dims=(((1,), (0,)), ((), ()))):
    return lax.dot_general(a, b, dims, preferred_element_type=F32)


def hot(mask):
    return jnp.where(mask, 1.0, 0.0).astype(BF16)


def spread_row():
    return hot(iota((32, 1024), 1) // 32 == iota((32, 1024), 0))


def spread_col():
    return hot(iota((32, 1024), 1) % 32 == iota((32, 1024), 0))


def fold_first(x):
    w = x[:, 0:128]
    for q in range(1, 8):
        w = w + x[:, q * 128 : (q + 1) * 128]
    return (w[:, 0:32] + w[:, 32:64]) + (w[:, 64:96] + w[:, 96:128])


def leaf_of(siz_ref, start, width):
    sizes = siz_ref[...].astype(F32)
    lower = iota((32, 32), 1) <= iota((32, 32), 0)
    ends = jnp.sum(jnp.where(lower, jnp.broadcast_to(sizes, (32, 32)), 0.0), axis=1, keepdims=True)
    pos = (iota((32, width), 1) + start).astype(F32)
    return jnp.sum(jnp.where(pos >= ends, 1.0, 0.0), axis=0, keepdims=True)


CH = 4096


def down_kernel(top, far, mor, siz, bas, lt, mt, out):
    erow, ecol = spread_row(), spread_col()
    back = hot(iota((1024, 32), 0) // 32 == iota((1024, 32), 1))
    xt = dot(top[...], ecol)
    p = jnp.concatenate([xt * mt[m : m + 1, :].astype(F32) for m in range(4)], axis=0)
    ph = p.astype(BF16)
    pl_ = (p - ph.astype(F32)).astype(BF16)
    mid = (dot(ph, back) + dot(pl_, back)).astype(BF16)
    tots = []
    for m in range(4):
        x = dot(mid[m * 16 : (m + 1) * 16], ecol)
        q = jnp.concatenate(
            [x * lt[m * 8 + l : m * 8 + l + 1, :].astype(F32) for l in range(8)], axis=0
        ).astype(BF16)
        tots.append((dot(q, back) + far[m * 128 : (m + 1) * 128, :]).astype(BF16))
    tot = jnp.concatenate(tots, axis=0)

    def chunk(c, acc):
        at = pl.multiple_of(c * CH, CH)
        m = mor[:, pl.ds(at, CH)]
        lo, hi = m & 255, m >> 8
        pick = hot(iota((256, CH), 0) == lo)
        wide = dot(tot, bas[:, pl.ds(at, CH)])
        leaf = jnp.broadcast_to(leaf_of(siz, at, CH), (16, CH))
        o = wide[0:16]
        for l in range(1, 32):
            o = jnp.where(leaf == l, wide[l * 16 : (l + 1) * 16], o)
        ob = o.astype(BF16)
        hib = jnp.broadcast_to(hi, (16, CH)).astype(F32).astype(BF16)
        scat = jnp.concatenate([jnp.where(hib == h, ob, jnp.zeros((), BF16)) for h in range(16)], axis=0)
        return acc + dot(scat, pick, NT)

    acc = lax.fori_loop(0, 4096 // CH, chunk, jnp.zeros((256, 256), F32), unroll=2)
    for h in range(16):
        out[:, h * 256 : (h + 1) * 256] = acc[h * 16 : (h + 1) * 16]


S = jax.ShapeDtypeStruct
VM = pltpu.VMEM


def down(top, far, mor, siz, bas, lt, mt):
    return pl.pallas_call(down_kernel, out_shape=S((16, 4096), F32))(top, far, mor, siz, bas, lt, mt)


AXES = ("leaf_0", "leaf_1", "leaf_2", "leaf_3")
MESH = pl.DeviceIdType.MESH


def split2(x):
    hi = x.astype(BF16)
    return hi, (x - hi.astype(F32)).astype(BF16)


def pack_row(c):
    wide = dot(c, hot(iota((32, 128), 1) % 32 == iota((32, 128), 0)))
    wide = jnp.where(iota((16, 128), 1) // 32 == iota((16, 128), 0) % 4, wide, 0.0).astype(BF16)
    return dot(hot(iota((4, 16), 1) // 4 == iota((4, 16), 0)), wide)


def unpack_row(r):
    sel = hot(iota((16, 4), 0) // 4 == iota((16, 4), 1))
    hi, lo = split2(r)
    wide = dot(sel, hi) + dot(sel, lo)
    wide = jnp.where(iota((16, 128), 1) // 32 == iota((16, 128), 0) % 4, wide, 0.0)
    return (wide[:, 0:32] + wide[:, 32:64]) + (wide[:, 64:96] + wide[:, 96:128])


def sum_rows(ref, n):
    flat = ref[...].reshape(n * 4, 128)
    return dot(hot(iota((4, n * 4), 1) % 4 == iota((4, n * 4), 0)), flat)


def back_weights(c, w):
    cex = dot(c, hot(iota((16, 512), 1) // 32 == iota((16, 512), 0)), TN)
    same = iota((32, 512), 1) % 32 == iota((32, 512), 0)
    for i in range(32):
        row = jnp.broadcast_to(cex[i : i + 1, :], (32, 512))
        w[i * 32 : (i + 1) * 32, :] = jnp.where(same, row, 0.0).astype(BF16)


def forward_sum(blocks, chosen):
    same = iota((32, 512), 1) % 32 == iota((32, 512), 0)
    rows = []
    for q in range(4):
        part = dot(blocks[:, q * 256 : (q + 1) * 256], chosen, TN)
        for i in range(8):
            rows.append(jnp.sum(jnp.where(same, part[i * 32 : (i + 1) * 32], 0.0), axis=0, keepdims=True))
    y = jnp.concatenate(rows, axis=0)
    hi, lo = split2(y)
    sel = hot(iota((16, 512), 1) // 32 == iota((16, 512), 0))
    return dot(sel, hi, NT) + dot(sel, lo, NT)


UP = 512


def lanes_of(x):
    return x.reshape(x.shape[0], 512)


def add_all(terms):
    return functools.reduce(lambda a, b: a + b, [t.astype(F32) for t in terms]).astype(BF16)


def mega_kernel(dims, *refs):
    ins, (top_out, far_out), rest = refs[:13], refs[13:15], refs[15:]
    staged, (inputs, *rest) = rest[:13], rest[13:]
    mega_body(dims, ins, staged, inputs, top_out, far_out, *rest)


def mega_body(dims, ins, staged, inputs, top_out, far_out,
                masked, lt32, lc, s32, idcol, leaf_far,
                ca, rsb, rx, sb, rx2, sb2, rr, gx, sgx, pgx, gcb, tb, gr2, tb2, gr, w,
                rowb, termb, pgs, gcrow, send, recv):
    loads = [pltpu.make_async_copy(a, b, inputs.at[i]) for i, (a, b) in enumerate(zip(ins, staged))]
    for load in loads:
        load.start()
    vec, mor, siz, bas, lt, mt, rt, pairs, lcoup, partner, dcoup, gpart, gcoup = staged
    nx, ny, nz = dims
    halves = nz // 4
    plane, pgs_n = ny * nz, ny * halves
    x, y, z, c = [lax.axis_index(a) for a in AXES]
    zq, zh = z % 4, z // 4
    k = zq * 2 + c
    yz = y * nz + z
    pg = y * halves + zh
    xs = [(x + j) % nx for j in range(nx)]
    ys = [(y + j) % ny for j in range(ny)]
    zs = [(z + j) % nz for j in range(nz)]
    gz = [((zh + j) % halves) * 4 + zq for j in range(halves)]
    far_first = lambda o: -(min(o[0], ny - o[0]) + min(o[1], nz - o[1]))
    offs = sorted([(a, b) for a in range(ny) for b in range(nz) if a or b], key=far_first)
    goffs = sorted([(a, b) for a in range(ny) for b in range(halves) if a or b], key=lambda o: -min(o[0], ny - o[0]))
    near_y = [a for a in range(ny) if min(a, ny - a) <= ny // 4]
    far_y = [a for a in range(ny) if a not in near_y]
    row_of = lambda a: pl.ds(ys[a] * nz, nz)
    sibling = (x, y, z, 1 - c)

    def mate(j):
        r = (k + j) % 8
        return (x, y, zh * 4 + r // 2, r % 2)

    def push(src, dst, i, to):
        pltpu.make_async_remote_copy(src, dst, send.at[i], recv.at[i], device_id=to, device_id_type=MESH).start()

    def settle(ref, i, which):
        cp = pltpu.make_async_remote_copy(
            ref, ref, send.at[i], recv.at[i], device_id=sibling, device_id_type=MESH
        )
        (cp.wait_recv if which else cp.wait_send)()

    def got(ref, i):
        settle(ref, i, True)

    def sent(ref, i):
        settle(ref, i, False)

    bar = pltpu.get_barrier_semaphore()

    def greet(to):
        pl.semaphore_signal(bar, inc=1, device_id=to, device_id_type=MESH)

    for a, b in offs:
        greet((x, ys[a], zs[b], c))
    for j in range(1, nx):
        greet((xs[j], y, z, c))
    for j in range(1, 8):

        @pl.when((k + j) % 2 != c)
        def _():
            greet(mate(j))

    for i in (0, 1, 2):
        loads[i].wait()
    vx = jnp.concatenate([vec[:, h * 256 : (h + 1) * 256] for h in range(16)], axis=0).astype(BF16)

    def chunk(i, carry):
        at = pl.multiple_of(i * UP, UP)
        m = mor[:, pl.ds(at, UP)]
        lo, hi = m & 255, m >> 8
        wide = dot(vx, hot(iota((256, UP), 0) == lo))
        hib = jnp.broadcast_to(hi, (16, UP))
        sv = wide[0:16]
        for h in range(1, 16):
            sv = jnp.where(hib == h, wide[h * 16 : (h + 1) * 16], sv)
        leaf = jnp.broadcast_to(leaf_of(siz, at, UP), (16, UP)).astype(BF16)
        svb = sv.astype(BF16)
        for l in range(32):
            masked[l * 16 : (l + 1) * 16, pl.ds(at, UP)] = jnp.where(leaf == l, svb, jnp.zeros((), BF16))
        return carry

    lax.fori_loop(0, 4096 // UP, chunk, 0, unroll=2)
    for load in loads[3:]:
        load.wait()
    pgs[...] = jnp.zeros((1, 128), I32)
    pgs[:, 0:4] = gpart[...]
    lt32[...] = lt[...].astype(F32)
    lcv = dot(bas[...], masked[...], NT).astype(BF16)
    lc[...] = lcv
    erow, ecol = spread_row(), spread_col()
    root = jnp.zeros((16, 1024), F32)
    for m in range(4):
        acc = jnp.zeros((16, 1024), F32)
        wide = dot(lcv[:, m * 128 : (m + 1) * 128], erow, TN)
        for l in range(8):
            acc = acc + wide[l * 16 : (l + 1) * 16] * lt32[m * 8 + l : m * 8 + l + 1, :]
        mid = fold_first(acc).astype(BF16)
        root = root + dot(mid, erow) * mt[m : m + 1, :].astype(F32)
    root = fold_first(root).astype(BF16)
    term = fold_first(dot(root, erow) * rt[...].astype(F32)).astype(BF16)
    rowb[...] = pack_row(root).astype(BF16)
    termb[...] = pack_row(term).astype(BF16)
    pl.semaphore_wait(bar, plane - 1 + nx - 1 + 4)

    for j in range(1, 8):
        push(termb, gx.at[k], 0, mate(j))
    for j in range(1, 8):
        push(gcoup, sgx.at[k], 1, mate(j))
        push(pgs, pgx.at[k], 2, mate(j))
    for a, b in offs:
        push(rowb, ca.at[c, x, yz], 3 if a in near_y else 9, (x, ys[a], zs[b], c))
    gx[k] = termb[...]
    sgx[k] = gcoup[...]
    pgx[k] = pgs[...]
    ca[c, x, yz] = rowb[...]

    back_weights(root, w)
    bk = dot(dcoup[...], w[...]).astype(BF16)
    chips = nx * plane
    for half in range(2):
        ids = iota((chips, 128), 0) * 2 + half
        hotb = hot(ids == jnp.broadcast_to(partner[...], (chips, 128)))
        rsb[half] = dot(hotb, bk).astype(BF16).reshape(nx, plane, 4, 128)
    push(rsb.at[1 - c], rx, 4, sibling)

    s32[...] = lcoup[...].astype(F32)
    back = hot(iota((1024, 32), 0) // 32 == iota((1024, 32), 1))
    each = hot(iota((64, 1024), 1) // 16 == iota((64, 1024), 0))
    idcol[...] = dot(each, pairs[...].astype(F32).astype(BF16), (((0,), (1,)), ((), ())))

    def leaf_group(gi):
        eye = iota((512, 512), 0) % 16 == iota((512, 512), 1) % 16
        lid = (iota((512, 512), 1) // 16).astype(F32)
        at = slice(gi * 512, gi * 512 + 512)
        first, second = [
            hot(eye & (jnp.broadcast_to(idcol[at, i : i + 1], (512, 512)) == lid)) for i in (0, 1)
        ]
        rows = [s32[gi * 32 + t : gi * 32 + t + 1, :] for t in range(32)]
        wide = dot(dot(second, lc[...], NT).astype(BF16), ecol)
        parts = [wide[t * 16 : (t + 1) * 16] * rows[t] for t in range(32)]
        forth = dot(jnp.concatenate(parts, axis=0).astype(BF16), back).astype(BF16)
        wide = dot(dot(first, lc[...], NT).astype(BF16), erow)
        parts = [fold_first(wide[t * 16 : (t + 1) * 16] * rows[t]) for t in range(32)]
        return dot(forth, first, TN) + dot(jnp.concatenate(parts, axis=0).astype(BF16), second, TN)

    leaf_far[...] = leaf_group(0)

    got(rx, 4)
    sb[...] = add_all([rsb[c], rx[...]])
    for part, i in ((far_y, 6), (near_y, 13 + nx)):
        for a in part:
            for j in range(1, nx):
                push(sb.at[xs[j], row_of(a)], rx2.at[j - 1, row_of(a)], i, (xs[j], y, z, c))

    got(gx.at[pl.ds(0, 7)], 0)
    gcoef = sum_rows(gx, 8).astype(BF16)
    gcrow[...] = gcoef
    for a, b in goffs:
        push(gcrow, gcb.at[x, pg], 5, (x, ys[a], gz[b], c))
    gcb[x, pg] = gcoef

    got(sgx.at[pl.ds(0, 7)], 1)
    got(pgx.at[pl.ds(0, 7)], 2)
    sg = sgx[...].reshape(32, 1024)
    groups = nx * pgs_n
    p8 = pgx[...].reshape(8, 128).astype(F32).astype(BF16)[:, 0:4]
    spread = dot(p8, hot(iota((4, 32), 1) % 4 == iota((4, 32), 0)))
    gpair = jnp.sum(jnp.where(iota((8, 32), 1) // 4 == iota((8, 32), 0), spread, 0.0), axis=0, keepdims=True)
    hotg = hot(iota((groups, 32), 0).astype(F32) == jnp.broadcast_to(gpair, (groups, 32)))

    back_weights(unpack_row(gcoef.astype(F32)).astype(BF16), w)
    tb[...] = dot(hotg, dot(sg, w[...]).astype(BF16)).astype(BF16).reshape(nx, pgs_n, 4, 128)
    for j in range(1, nx):
        push(tb.at[xs[j]], gr2.at[j - 1], 7, (xs[j], y, z, c))

    def along_x(part):
        for a in part:
            for j in range(1, nx):
                push(ca.at[c, x, row_of(a)], ca.at[c, x, row_of(a)], 13 + j, (xs[j], y, z, c))

    got(ca.at[c, x, pl.ds(0, len(near_y) * nz - 1)], 3)
    along_x(near_y)
    got(ca.at[c, x, pl.ds(0, len(far_y) * nz)], 9)
    along_x(far_y)
    push(ca.at[c, x], ca.at[c, x], 8, sibling)

    def over_plane(part, i):
        got(rx2.at[:, pl.ds(0, len(part) * nz)], i)
        for a in part:
            sb2[row_of(a)] = add_all([sb[x, row_of(a)]] + [rx2[j, row_of(a)] for j in range(nx - 1)])
        for a, b in offs:
            if a in part:
                push(sb2.at[ys[a] * nz + zs[b]], rr.at[yz], 10, (x, ys[a], zs[b], c))

    over_plane(far_y, 6)
    got(gr2, 7)
    tb2[...] = add_all([tb[x]] + [gr2[j] for j in range(nx - 1)])
    for a, b in goffs:
        push(tb2.at[ys[a] * halves + (zh + b) % halves], gr.at[pg], 11, (x, ys[a], gz[b], c))
    gr[pg] = tb2[pg]
    over_plane(near_y, 13 + nx)
    rr[yz] = sb2[yz]

    leaf_far[...] += leaf_group(1)

    for j in sorted(range(1, nx), key=lambda j: min(j, nx - j)):
        got(ca.at[c, x], 13 + j)
        push(ca.at[c, xs[-j]], ca.at[c, xs[-j]], 13, sibling)
    got(gcb.at[x, pl.ds(0, pgs_n - 1)], 5)
    for j in range(1, nx):
        push(gcb.at[x], gcb.at[x], 12, (xs[j], y, z, c))
    far_out[...] = leaf_far[...].T
    got(ca.at[c, x], 8)
    got(ca.at[c, pl.ds(0, nx - 1)], 13)
    near = jnp.zeros((128, 512), F32)
    for half in range(2):
        ids = iota((chips, 128), 0) * 2 + half
        hotb = hot(ids == jnp.broadcast_to(partner[...], (chips, 128)))
        near = near + dot(hotb, lanes_of(ca[half].reshape(chips, 4, 128)), TN)
    root_far = forward_sum(dcoup[...], near.astype(BF16))
    got(gcb.at[pl.ds(0, nx - 1)], 12)
    far = dot(hotg, lanes_of(gcb[...].reshape(groups, 4, 128)), TN).astype(BF16)
    group_far = forward_sum(sg, far)
    got(gr.at[pl.ds(0, pgs_n - 1)], 11)
    group_far = (group_far + unpack_row(sum_rows(gr, pgs_n))).astype(BF16)
    got(rr.at[pl.ds(0, plane - 1)], 10)
    root_far = root_far + unpack_row(sum_rows(rr, plane))
    hi, lo = split2(dot(group_far, ecol) * rt[...].astype(F32))
    top_out[...] = (root_far + dot(hi, back) + dot(lo, back)).astype(BF16)

    sent(gx.at[pl.ds(0, 7)], 0)
    sent(sgx.at[pl.ds(0, 7)], 1)
    sent(pgx.at[pl.ds(0, 7)], 2)
    sent(ca.at[c, x, pl.ds(0, len(near_y) * nz - 1)], 3)
    sent(ca.at[c, x, pl.ds(0, len(far_y) * nz)], 9)
    sent(rx, 4)
    sent(gcb.at[x, pl.ds(0, pgs_n - 1)], 5)
    sent(rx2.at[:, pl.ds(0, len(far_y) * nz)], 6)
    sent(rx2.at[:, pl.ds(0, len(near_y) * nz)], 13 + nx)
    sent(gr2, 7)
    sent(ca.at[c, x], 8)
    for j in range(1, nx):
        sent(ca.at[c, x], 13 + j)
    sent(rr.at[pl.ds(0, plane - 1)], 10)
    sent(gr.at[pl.ds(0, pgs_n - 1)], 11)
    sent(gcb.at[pl.ds(0, nx - 1)], 12)
    sent(ca.at[c, pl.ds(0, nx - 1)], 13)


def mega(dims, vec, mor, siz, bas, lt, mt, rt, pairs, lcoup, partner, dcoup, gpart, gcoup):
    nx, ny, nz = dims
    plane, pgn = ny * nz, ny * nz // 4
    b = lambda *s: pltpu.VMEM(s, BF16)
    ins = (vec, mor, siz, bas, lt, mt, rt, pairs, lcoup, partner, dcoup, gpart, gcoup)
    scratch = [
        b(512, 4096), VM((32, 1024), F32), b(32, 512), VM((64, 1024), F32), VM((1024, 2), F32), VM((32, 512), F32),
        b(2, nx, plane, 4, 128), b(2, nx, plane, 4, 128), b(nx, plane, 4, 128), b(nx, plane, 4, 128),
        b(nx - 1, plane, 4, 128), b(plane, 4, 128), b(plane, 4, 128),
        b(8, 4, 128), b(8, 4, 1024), VM((8, 1, 128), I32),
        b(nx, pgn, 4, 128), b(nx, pgn, 4, 128), b(nx - 1, pgn, 4, 128), b(pgn, 4, 128), b(pgn, 4, 128),
        b(1024, 512), b(4, 128), b(4, 128), VM((1, 128), I32), b(4, 128),
        pltpu.SemaphoreType.DMA((14 + nx,)), pltpu.SemaphoreType.DMA((14 + nx,)),
    ]
    return pl.pallas_call(
        functools.partial(mega_kernel, dims),
        out_shape=(S((16, 32), BF16), S((512, 32), F32)),
        in_specs=[pl.BlockSpec(memory_space=pl.ANY)] * 13,
        scratch_shapes=[VM(a.shape, a.dtype) for a in ins] + [pltpu.SemaphoreType.DMA((13,))] + scratch,
        compiler_params=pltpu.CompilerParams(collective_id=0, has_side_effects=True),
    )(*ins)


def body(dims, vec, mor, siz, bas, lt, mt, rt, pairs, lcoup, partner, dcoup, gpart, gcoup):
    top, far = mega(dims, vec, mor, siz, bas, lt, mt, rt, pairs, lcoup, partner, dcoup, gpart, gcoup)
    return down(top, far, mor, siz, bas, lt, mt)


def solution(mesh):
    split = Mesh(mesh.devices.reshape(4, 8, 8, 2), AXES)
    rows, cols = P(AXES, None), P(None, AXES)
    in_specs = (cols, rows, rows, cols, rows, rows, rows, cols, rows, rows, rows, rows, rows)
    step = functools.partial(body, (4, 8, 8))
    return jax.shard_map(step, mesh=split, in_specs=in_specs, out_specs=cols, check_vma=False)
```
